32 devices in a mesh: batch: 1 (over z), gz: 4 (over y), gy: 4 (over x), gx: 2 (over core).
Axes of the slice: x: 4, y: 4, z: 1, core: 2. Of those that a mesh axis runs over, the one named last changes fastest.
The devices are a block of a 4x4x8 slice.
Arguments:
- u_init: float32 [64, 256, 256], P(('batch', 'gx'), 'gy', 'gz')
- f_rhs: float32 [64, 256, 256], P(('batch', 'gx'), 'gy', 'gz')
- kappa_cell: float32 [64, 256, 256], P(('batch', 'gx'), 'gy', 'gz')
- stencil_w: float32 [26], replicated
- omega_sweep: float32 [32], replicated
Outputs:
- output: float32 [64, 256, 256], P(('batch', 'gx'), 'gy', 'gz')
All inputs are finite; a program needn't handle non-finite values.
Results may differ from the reference program's by a relative error of at most 0.001.
Values are sent between devices in bfloat16 or wider.
A program may use at most 768 MiB of HBM per device.

```python
import math
import jax
import jax.numpy as jnp
from jax import lax

GRID_X = 64
GRID_Y = 256
GRID_Z = 256
SWEEPS = 32


def offset_list():
    unit_steps = (-1, 0, 1)
    return [(a, b, c) for a in unit_steps for b in unit_steps for c in unit_steps if (a, b, c) != (0, 0, 0)]


def shifted(array_in, offset):
    return jnp.roll(array_in, (-offset[0], -offset[1], -offset[2]), axis=(0, 1, 2))


def setup_inputs(seed: int = 0, part: int = 0) -> dict:
    root_key = jax.random.key(seed)
    shared_key, part_root = jax.random.split(root_key)
    part_key = jax.random.fold_in(part_root, part)
    key_u, key_f, key_kappa = jax.random.split(part_key, 3)
    key_w, key_omega = jax.random.split(shared_key)
    grid_shape = (GRID_X, GRID_Y, GRID_Z)
    u_init = jax.random.normal(key_u, grid_shape, jnp.float32)
    f_rhs = 30.0 * jax.random.normal(key_f, grid_shape, jnp.float32)
    kappa_cell = jnp.exp(jax.random.uniform(key_kappa, grid_shape, jnp.float32, 0.0, math.log(10.0)))
    stencil_w = jax.random.uniform(key_w, (26,), jnp.float32, 0.5, 1.5)
    omega_sweep = jax.random.uniform(key_omega, (SWEEPS,), jnp.float32, 0.6, 1.0)
    return dict(u_init=u_init, f_rhs=f_rhs, kappa_cell=kappa_cell, stencil_w=stencil_w, omega_sweep=omega_sweep)


def reference(u_init, f_rhs, kappa_cell, stencil_w, omega_sweep):
    offsets = offset_list()
    diag_total = jnp.zeros_like(kappa_cell)
    for w_idx, offset in enumerate(offsets):
        diag_total = diag_total + stencil_w[w_idx] * (0.5 * (kappa_cell + shifted(kappa_cell, offset)))

    def sweep_once(u_cur, relax_now):
        applied = jnp.zeros_like(u_cur)
        for w_idx, offset in enumerate(offsets):
            coef_io = stencil_w[w_idx] * (0.5 * (kappa_cell + shifted(kappa_cell, offset)))
            applied = applied + coef_io * (u_cur - shifted(u_cur, offset))
        return u_cur + relax_now * (f_rhs - applied) / diag_total, None

    u_final, unused = lax.scan(sweep_once, u_init, omega_sweep)
    return u_final
```

```python
import functools

import jax
import jax.numpy as jnp
from jax import lax
from jax.experimental import pallas as pl
from jax.experimental.pallas import tpu as pltpu
from jax.sharding import PartitionSpec as P

MESH = pl.DeviceIdType.MESH
F32 = jnp.float32
DEPTH = 4
ROW0 = 8
LANES = 128

OFFSETS = [(b, c, a) for a in (-1, 0, 1) for b in (-1, 0, 1) for c in (-1, 0, 1) if (a, b, c) != (0, 0, 0)]


def lane_of(shape):
    return lax.broadcasted_iota(jnp.int32, shape, len(shape) - 1)


def shift_x(v, c, half):
    lane = lane_of(v.shape) % half
    if c == 1:
        return jnp.where(lane == half - 1, pltpu.roll(v, half - 1, 1), pltpu.roll(v, 2 * half - 1, 1))
    return jnp.where(lane == 0, pltpu.roll(v, half + 1, 1), pltpu.roll(v, 1, 1))


def kernel(dims, u_in, f_in, k_in, w_ref, om_ref, out_ref,
           start0, start1, temp, kap, frc, coef, zsend, zrecv, drecv, send_sem, recv_sem):
    n_y, n_z, ny, nz, sweeps, tiles = dims
    s = DEPTH
    half = LANES // 2
    lo, hi = ROW0, ROW0 + nz
    qe = ny + 2 * s
    first = lo - s + 1

    core = lax.axis_index("gx")
    gy = lax.axis_index("gy")
    gz = lax.axis_index("gz")
    zhi, zlo = lax.rem(gz + 1, n_z), lax.rem(gz + n_z - 1, n_z)
    other = 1 - core
    yhi = lax.rem(gy + core, n_y)
    ylo = lax.rem(gy + n_y - other, n_y)

    def dev(y, z):
        if y is None:
            return {"gz": z}
        if z is None:
            return {"gx": other, "gy": y}
        return {"gx": other, "gy": y, "gz": z}

    neighbours = [dev(yhi, None), dev(ylo, None), dev(None, zhi), dev(None, zlo),
                  dev(yhi, zhi), dev(ylo, zhi), dev(yhi, zlo), dev(ylo, zlo)]

    barrier = pltpu.get_barrier_semaphore()
    for nb in neighbours:
        pl.semaphore_signal(barrier, inc=1, device_id=nb, device_id_type=MESH)

    hq = ny // 2

    def copies(arr, slot):
        pieces = [
            (arr.at[pl.ds(ny, s), pl.ds(lo, nz)], arr.at[pl.ds(0, s), pl.ds(lo, nz)]),
            (arr.at[pl.ds(s, s), pl.ds(lo, nz)], arr.at[pl.ds(ny + s, s), pl.ds(lo, nz)]),
            (zsend.at[slot, 0], zrecv.at[slot, 0]),
            (zsend.at[slot, 1], zrecv.at[slot, 1]),
            (zsend.at[slot, 0, pl.ds((hq - s) * s, s * s)], drecv.at[slot, 0]),
            (zsend.at[slot, 0, pl.ds(0, s * s)], drecv.at[slot, 1]),
            (zsend.at[slot, 1, pl.ds((hq - s) * s, s * s)], drecv.at[slot, 2]),
            (zsend.at[slot, 1, pl.ds(0, s * s)], drecv.at[slot, 3]),
        ]
        return [
            pltpu.make_async_remote_copy(
                src_ref=src, dst_ref=dst, send_sem=send_sem.at[slot, i], recv_sem=recv_sem.at[slot, i],
                device_id=neighbours[i], device_id_type=MESH)
            for i, (src, dst) in enumerate(pieces)
        ]

    left = lane_of((s, LANES)) < half

    def swap(v):
        return pltpu.roll(v, half, 1)

    def begin(arr, slot):
        for q in range(hq):
            top = jnp.where(left, swap(arr[s + q, pl.ds(hi - s, s)]), arr[s + q + hq, pl.ds(hi - s, s)])
            zsend[slot, 0, pl.ds(q * s, s)] = top
            bottom = jnp.where(left, arr[s + q, pl.ds(lo, s)], swap(arr[s + q + hq, pl.ds(lo, s)]))
            zsend[slot, 1, pl.ds(q * s, s)] = bottom
        for cp in copies(arr, slot):
            cp.start()

    def finish(arr, slot):
        for cp in copies(arr, slot):
            cp.wait()
        for q in range(qe):
            if q < s:
                low = swap(drecv[slot, 0, pl.ds(q * s, s)])
                high = drecv[slot, 2, pl.ds(q * s, s)]
            elif q < s + hq:
                low = zrecv[slot, 0, pl.ds((q - s) * s, s)]
                high = swap(zrecv[slot, 1, pl.ds((q - s) * s, s)])
            elif q < s + ny:
                low = swap(zrecv[slot, 0, pl.ds((q - s - hq) * s, s)])
                high = zrecv[slot, 1, pl.ds((q - s - hq) * s, s)]
            else:
                low = drecv[slot, 1, pl.ds((q - s - ny) * s, s)]
                high = swap(drecv[slot, 3, pl.ds((q - s - ny) * s, s)])
            arr[q, pl.ds(lo - s, s)] = jnp.where(left, low, swap(arr[q, pl.ds(hi - s, s)]))
            arr[q, pl.ds(hi, s)] = jnp.where(left, swap(arr[q, pl.ds(lo, s)]), high)

    for arr, src in ((start0, u_in), (kap, k_in), (frc, f_in)):
        @pl.loop(0, ny)
        def _(q, arr=arr, src=src):
            arr[s + q, pl.ds(lo, nz)] = src[q]
    pl.semaphore_wait(barrier, len(neighbours))
    begin(kap, 2)
    begin(frc, 3)
    begin(start0, 0)
    finish(kap, 2)
    finish(frc, 3)

    @pl.loop(1, qe - 1)
    def _(q):
        for t in range(tiles):
            base = first + 8 * t
            k_ab = {(a, b): kap[q + a, pl.ds(base + b, 8)] for a in (-1, 0, 1) for b in (-1, 0, 1)}
            k_mid = k_ab[0, 0]
            mids = {0: k_mid, 1: shift_x(k_mid, -1, half), -1: shift_x(k_mid, 1, half)}
            raw, sums = [], {}
            for m, (a, b, c) in enumerate(OFFSETS):
                d = (0.5 * w_ref[m]) * (mids[c] + k_ab[a, b])
                raw.append(d)
                sums[c] = d if c not in sums else sums[c] + d
            diag = sums[0] + shift_x(sums[1], 1, half) + shift_x(sums[-1], -1, half)
            inv = 1.0 / diag
            invs = {0: inv, 1: shift_x(inv, -1, half), -1: shift_x(inv, 1, half)}
            idx = (q - 1) * tiles + t
            for m, (a, b, c) in enumerate(OFFSETS):
                coef[idx, m] = raw[m] * invs[c]
            coef[idx, len(OFFSETS)] = frc[q, pl.ds(base, 8)] * inv

    BLOCK = 2

    def sweep(src, dst, j, relax):
        @pl.loop(0, (qe - 2 - 2 * j) // BLOCK)
        def _(blk):
            q0 = 1 + j + blk * BLOCK
            for t in range(tiles):
                base = first + 8 * t
                rows = {(i, b): src[q0 - 1 + i, pl.ds(base + b, 8)] for i in range(BLOCK + 2) for b in (-1, 0, 1)}
                for i in range(BLOCK):
                    idx = (q0 + i - 1) * tiles + t
                    sums = {0: coef[idx, len(OFFSETS)]}
                    for m, (a, b, c) in enumerate(OFFSETS):
                        p = coef[idx, m] * rows[i + 1 + a, b]
                        sums[c] = p if c not in sums else sums[c] + p
                    total = sums[0] + shift_x(sums[1], 1, half) + shift_x(sums[-1], -1, half)
                    mid = rows[i + 1, 0]
                    dst[q0 + i, pl.ds(base, 8)] = mid + relax * (total - mid)

    def group(arr, nxt, k0):
        bufs = [arr, temp]
        for j in range(s):
            dst = nxt if j == s - 1 else bufs[(j + 1) % 2]
            sweep(bufs[j % 2], dst, j, om_ref[k0 + j])

    groups = sweeps // s

    @pl.loop(0, groups // 2)
    def _(i):
        finish(start0, 0)
        group(start0, start1, 2 * s * i)
        begin(start1, 1)
        finish(start1, 1)
        group(start1, start0, 2 * s * i + s)

        @pl.when(i < groups // 2 - 1)
        def _():
            begin(start0, 0)

    @pl.loop(0, ny)
    def _(q):
        out_ref[q] = start0[s + q, pl.ds(lo, nz)]


def solution(mesh):
    spec = P(("batch", "gx"), "gy", "gz")
    n_x, n_y, n_z = mesh.shape["gx"], mesh.shape["gy"], mesh.shape["gz"]

    def local(u, f, k, w, om):
        bx, by, bz = u.shape
        ny, nz = by // n_x, bz // 2
        s = DEPTH
        tiles = -(-(nz + 2 * s - 2) // 8)
        rows = ROW0 + -(-(nz + s) // 8) * 8
        qe = ny + 2 * s

        def to_lanes(v):
            v = lax.all_to_all(v, "gx", 2, 1, tiled=True)
            v = v.reshape(3, bx * n_x, ny, 2, nz)
            return v.transpose(0, 2, 4, 3, 1).reshape(3, ny, nz, LANES)

        def from_lanes(v):
            v = v.reshape(ny, nz, 2, bx * n_x).transpose(3, 0, 2, 1).reshape(bx * n_x, ny, bz)
            return lax.all_to_all(v, "gx", 0, 1, tiled=True)

        packed = to_lanes(jnp.stack([u, f, k]))
        vm = pl.BlockSpec(memory_space=pltpu.VMEM)
        sm = pl.BlockSpec(memory_space=pltpu.SMEM)
        arr = pltpu.VMEM((qe, rows, LANES), F32)
        out = pl.pallas_call(
            functools.partial(kernel, (n_y, n_z, ny, nz, om.shape[0], tiles)),
            out_shape=jax.ShapeDtypeStruct((ny, nz, LANES), F32),
            in_specs=[vm, vm, vm, sm, sm],
            out_specs=vm,
            scratch_shapes=[
                arr, arr, arr, arr, arr,
                pltpu.VMEM(((qe - 2) * tiles, len(OFFSETS) + 1, 8, LANES), F32),
                pltpu.VMEM((4, 2, ny // 2 * s, LANES), F32),
                pltpu.VMEM((4, 2, ny // 2 * s, LANES), F32),
                pltpu.VMEM((4, 4, s * s, LANES), F32),
                pltpu.SemaphoreType.DMA((4, 8)),
                pltpu.SemaphoreType.DMA((4, 8)),
            ],
            compiler_params=pltpu.CompilerParams(collective_id=0, has_side_effects=True, vmem_limit_bytes=56 << 20),
        )(packed[0], packed[1], packed[2], w, om)
        return from_lanes(out)

    return jax.shard_map(local, mesh=mesh, in_specs=(spec, spec, spec, P(), P()), out_specs=spec, check_vma=False)
```

```python
import functools

import jax
import jax.numpy as jnp
from jax import lax
from jax.experimental import pallas as pl
from jax.experimental.pallas import tpu as pltpu
from jax.sharding import PartitionSpec as P

MESH = pl.DeviceIdType.MESH
F32 = jnp.float32
DEPTH = 4
ROW0 = 8
LANES = 128

OFFSETS = [(b, c, a) for a in (-1, 0, 1) for b in (-1, 0, 1) for c in (-1, 0, 1) if (a, b, c) != (0, 0, 0)]


def lane_of(shape):
    return lax.broadcasted_iota(jnp.int32, shape, len(shape) - 1)


def repeat(count, body):
    lax.fori_loop(0, count, lambda i, carry: (body(i), carry)[1], 0, unroll=count)


def shift_x(v, c, half):
    lane = lane_of(v.shape) % half
    if c == 1:
        return jnp.where(lane == half - 1, pltpu.roll(v, half - 1, v.ndim - 1), pltpu.roll(v, 2 * half - 1, v.ndim - 1))
    return jnp.where(lane == 0, pltpu.roll(v, half + 1, v.ndim - 1), pltpu.roll(v, 1, v.ndim - 1))


def kernel(dims, u_in, f_in, k_in, w_ref, om_ref, out_ref,
           ext, temp, coef, nat, zsend, zrecv, drecv,
           send_sem, recv_sem, here_sem, pair_send, pair_recv):
    n_y, n_z, ny, nz, sweeps, tiles = dims
    s = DEPTH
    half = LANES // 2
    lo, hi = ROW0, ROW0 + nz
    qe = ny + 2 * s
    first = lo - s + 1
    bx = u_in.shape[0]

    core = lax.axis_index("gx")
    gy = lax.axis_index("gy")
    gz = lax.axis_index("gz")
    zhi, zlo = lax.rem(gz + 1, n_z), lax.rem(gz + n_z - 1, n_z)
    other = 1 - core
    yhi = lax.rem(gy + core, n_y)
    ylo = lax.rem(gy + n_y - other, n_y)

    neighbours = [
        {"gx": other, "gy": yhi, "gz": zhi}, {"gx": other, "gy": ylo, "gz": zhi},
        {"gx": other, "gy": yhi, "gz": zlo}, {"gx": other, "gy": ylo, "gz": zlo},
        {"gz": zhi}, {"gz": zlo}, {"gx": other, "gy": yhi}, {"gx": other, "gy": ylo},
    ]

    barrier = pltpu.get_barrier_semaphore()
    for nb in neighbours:
        pl.semaphore_signal(barrier, inc=1, device_id=nb, device_id_type=MESH)

    mine = pl.multiple_of(core * ny, ny)
    theirs = pl.multiple_of(other * ny, ny)
    my_x = pl.ds(core * bx, bx)
    kap, frc = 2, 3
    fields = (u_in, k_in, f_in)
    kept = [pltpu.make_async_copy(src.at[:, pl.ds(mine, ny)], nat.at[i, my_x], here_sem.at[i])
            for i, src in enumerate(fields)]
    given = [pltpu.make_async_remote_copy(
        src_ref=src.at[:, pl.ds(theirs, ny)], dst_ref=nat.at[i, my_x], send_sem=pair_send.at[i],
        recv_sem=pair_recv.at[i], device_id={"gx": other}, device_id_type=MESH)
        for i, src in enumerate(fields)]
    for i in (1, 2, 0):
        kept[i].start()

    hq = ny // 2

    def copies(arr, slot):
        pieces = [
            (zsend.at[slot, 0, pl.ds((hq - s) * s, s * s)], drecv.at[slot, 0]),
            (zsend.at[slot, 0, pl.ds(0, s * s)], drecv.at[slot, 1]),
            (zsend.at[slot, 1, pl.ds((hq - s) * s, s * s)], drecv.at[slot, 2]),
            (zsend.at[slot, 1, pl.ds(0, s * s)], drecv.at[slot, 3]),
            (zsend.at[slot, 0], zrecv.at[slot, 0]),
            (zsend.at[slot, 1], zrecv.at[slot, 1]),
            (ext.at[arr, pl.ds(ny, s), pl.ds(lo, nz)], ext.at[arr, pl.ds(0, s), pl.ds(lo, nz)]),
            (ext.at[arr, pl.ds(s, s), pl.ds(lo, nz)], ext.at[arr, pl.ds(ny + s, s), pl.ds(lo, nz)]),
        ]
        return [
            pltpu.make_async_remote_copy(
                src_ref=src, dst_ref=dst, send_sem=send_sem.at[slot, i], recv_sem=recv_sem.at[slot, i],
                device_id=neighbours[i], device_id_type=MESH)
            for i, (src, dst) in enumerate(pieces)
        ]

    left = lane_of((s, LANES)) < half

    def swap(v):
        return pltpu.roll(v, half, 1)

    def begin(arr, slot):
        def pack(q):
            top = jnp.where(left, swap(ext[arr, s + q, pl.ds(hi - s, s)]), ext[arr, s + q + hq, pl.ds(hi - s, s)])
            zsend[slot, 0, pl.ds(q * s, s)] = top
            bottom = jnp.where(left, ext[arr, s + q, pl.ds(lo, s)], swap(ext[arr, s + q + hq, pl.ds(lo, s)]))
            zsend[slot, 1, pl.ds(q * s, s)] = bottom

        repeat(hq, pack)
        for cp in copies(arr, slot):
            cp.start()

    def finish(arr, slot):
        for cp in copies(arr, slot):
            cp.wait()
        def fill(q, low, high):
            ext[arr, q, pl.ds(lo - s, s)] = jnp.where(left, low, swap(ext[arr, q, pl.ds(hi - s, s)]))
            ext[arr, q, pl.ds(hi, s)] = jnp.where(left, swap(ext[arr, q, pl.ds(lo, s)]), high)

        def at(ref, i, q):
            return ref[slot, i, pl.ds(q * s, s)]

        repeat(s, lambda q: fill(q, swap(at(drecv, 0, q)), at(drecv, 2, q)))
        repeat(hq, lambda q: fill(s + q, at(zrecv, 0, q), swap(at(zrecv, 1, q))))
        repeat(hq, lambda q: fill(s + hq + q, swap(at(zrecv, 0, q)), at(zrecv, 1, q)))
        repeat(s, lambda q: fill(s + ny + q, at(drecv, 1, q), swap(at(drecv, 3, q))))

    pl.semaphore_wait(barrier, len(neighbours))
    for i in (1, 2, 0):
        given[i].start()

    @pl.loop(0, 3)
    def _(turn):
        i = lax.rem(turn + 1, 3)
        arr = i + lax.div(i + 1, 2)
        pltpu.make_async_copy(u_in.at[:, pl.ds(mine, ny)], nat.at[i, my_x], here_sem.at[i]).wait()
        pltpu.make_async_remote_copy(
            src_ref=u_in.at[:, pl.ds(theirs, ny)], dst_ref=nat.at[i, my_x], send_sem=pair_send.at[i],
            recv_sem=pair_recv.at[i], device_id={"gx": other}, device_id_type=MESH).wait()

        @pl.loop(0, ny // 8)
        def _(yt):
            y0 = pl.multiple_of(yt * 8, 8)
            planes = jnp.swapaxes(nat[i, :, pl.ds(y0, 8), :], 0, 1)
            for y in range(8):
                turned = planes[y].T
                ext[arr, s + y0 + y, pl.ds(lo, nz)] = jnp.concatenate([turned[:nz], turned[nz:]], axis=1)

        begin(arr, arr)

    @pl.loop(kap, frc + 1)
    def _(arr):
        finish(arr, arr)

    @pl.loop(1, qe - 1)
    def _(q):
        def tile(t):
            base = first + 8 * t
            k_ab = {(a, b): ext[kap, q + a, pl.ds(base + b, 8)] for a in (-1, 0, 1) for b in (-1, 0, 1)}
            k_mid = k_ab[0, 0]
            mids = {0: k_mid, 1: shift_x(k_mid, -1, half), -1: shift_x(k_mid, 1, half)}
            raw, sums = [], {}
            for m, (a, b, c) in enumerate(OFFSETS):
                d = (0.5 * w_ref[m]) * (mids[c] + k_ab[a, b])
                raw.append(d)
                sums[c] = d if c not in sums else sums[c] + d
            diag = sums[0] + shift_x(sums[1], 1, half) + shift_x(sums[-1], -1, half)
            inv = 1.0 / diag
            invs = {0: inv, 1: shift_x(inv, -1, half), -1: shift_x(inv, 1, half)}
            for m, (a, b, c) in enumerate(OFFSETS):
                coef[q - 1, t, m] = raw[m] * invs[c]
            coef[q - 1, t, len(OFFSETS)] = ext[frc, q, pl.ds(base, 8)] * inv

        repeat(tiles, tile)

    def update(src, dst, relax, q_lo, q_hi, which, unroll):
        def block(q0, n):
            for t in which:
                base = first + 8 * t
                rows = {b: src[pl.ds(q0 - 1, n + 2), pl.ds(base + b, 8)] for b in (-1, 0, 1)}
                sums = {0: coef[pl.ds(q0 - 1, n), t, len(OFFSETS)]}
                for m, (a, b, c) in enumerate(OFFSETS):
                    p = coef[pl.ds(q0 - 1, n), t, m] * rows[b][1 + a:1 + a + n]
                    sums[c] = p if c not in sums else sums[c] + p
                total = sums[0] + shift_x(sums[1], 1, half) + shift_x(sums[-1], -1, half)
                mid = rows[0][1:1 + n]
                dst[pl.ds(q0, n), pl.ds(base, 8)] = mid + relax * (total - mid)

        count = q_hi - q_lo
        if count // unroll == 1:
            block(q_lo, unroll)
        elif count >= unroll:
            @pl.loop(0, count // unroll)
            def _(blk):
                block(q_lo + blk * unroll, unroll)

        if count % unroll:
            block(q_lo + count // unroll * unroll, count % unroll)

    every = tuple(range(tiles))
    inner_first = tuple(t for t in every if first + 8 * t > lo and first + 8 * t + 8 < hi)
    outer_first = tuple(t for t in every if t not in inner_first)
    inner_last = tuple(t for t in every if first + 8 * t >= lo + s and first + 8 * t + 8 <= hi - s)
    outer_last = tuple(t for t in every if t not in inner_last)

    def group(slot, k0, send):
        arr, nxt = ext.at[slot], ext.at[1 - slot]
        relax = om_ref[k0]
        update(arr, temp, relax, s + 1, s + ny - 1, inner_first, 6)
        finish(slot, slot)
        update(arr, temp, relax, 1, s + 1, every, 4)
        update(arr, temp, relax, s + 1, s + ny - 1, outer_first, 6)
        update(arr, temp, relax, s + ny - 1, qe - 1, every, 4)
        bufs = [arr, temp]
        for j in range(1, s - 1):
            update(bufs[j % 2], bufs[(j + 1) % 2], om_ref[k0 + j], 1 + j, qe - 1 - j, every, 4)
        src, relax = bufs[(s - 1) % 2], om_ref[k0 + s - 1]
        update(src, nxt, relax, s, 2 * s, every, 4)
        update(src, nxt, relax, ny, ny + s, every, 4)
        update(src, nxt, relax, 2 * s, ny, outer_last, 4)
        send()
        update(src, nxt, relax, 2 * s, ny, inner_last, 6)

    groups = sweeps // s

    @pl.loop(0, groups)
    def _(i):
        slot = lax.rem(i, 2)

        def send():
            @pl.when(i < groups - 1)
            def _():
                begin(1 - slot, 1 - slot)

        group(slot, s * i, send)

    last = groups % 2

    def home(yt):
        rows = pl.ds(pl.multiple_of(core * ny + yt * 8, 8), 8)
        return (pltpu.make_async_copy(
                    nat.at[0, my_x, pl.ds(pl.multiple_of(yt * 8, 8), 8)], out_ref.at[:, rows], here_sem.at[yt]),
                pltpu.make_async_remote_copy(
                    src_ref=nat.at[0, pl.ds(other * bx, bx), pl.ds(pl.multiple_of(yt * 8, 8), 8)], dst_ref=out_ref.at[:, rows],
                    send_sem=pair_send.at[yt], recv_sem=pair_recv.at[yt], device_id={"gx": other},
                    device_id_type=MESH))

    @pl.loop(0, ny // 8)
    def _(step):
        yt = pl.multiple_of(step * 8, 8)
        planes = []
        for y in range(8):
            row = ext[last, s + yt + y, pl.ds(lo, nz)]
            planes.append(jnp.concatenate([row[:, :half], row[:, half:]], axis=0).T)
        nat[0, :, pl.ds(yt, 8), :] = jnp.swapaxes(jnp.stack(planes), 0, 1)
        for cp in home(step):
            cp.start()

    @pl.loop(0, ny // 8)
    def _(step):
        for cp in home(step):
            cp.wait()


def solution(mesh):
    spec = P(("batch", "gx"), "gy", "gz")
    n_x, n_y, n_z = mesh.shape["gx"], mesh.shape["gy"], mesh.shape["gz"]

    def local(u, f, k, w, om):
        bx, by, bz = u.shape
        ny, nz = by // n_x, bz // 2
        s = DEPTH
        tiles = -(-(nz + 2 * s - 2) // 8)
        rows = ROW0 + -(-(nz + s) // 8) * 8
        qe = ny + 2 * s
        hbm = pl.BlockSpec(memory_space=pl.ANY)
        sm = pl.BlockSpec(memory_space=pltpu.SMEM)
        dma = pltpu.SemaphoreType.DMA
        return pl.pallas_call(
            functools.partial(kernel, (n_y, n_z, ny, nz, om.shape[0], tiles)),
            out_shape=jax.ShapeDtypeStruct(u.shape, F32),
            in_specs=[hbm, hbm, hbm, sm, sm],
            out_specs=hbm,
            scratch_shapes=[
                pltpu.VMEM((4, qe, rows, LANES), F32),
                pltpu.VMEM((qe, rows, LANES), F32),
                pltpu.VMEM((qe - 2, tiles, len(OFFSETS) + 2, 8, LANES), F32),
                pltpu.VMEM((3, n_x * bx, ny, bz), F32),
                pltpu.VMEM((4, 2, ny // 2 * s, LANES), F32),
                pltpu.VMEM((4, 2, ny // 2 * s, LANES), F32),
                pltpu.VMEM((4, 4, s * s, LANES), F32),
                dma((4, 8)), dma((4, 8)), dma((4,)), dma((4,)), dma((4,)),
            ],
            compiler_params=pltpu.CompilerParams(collective_id=0, has_side_effects=True, vmem_limit_bytes=56 << 20),
        )(u, f, k, w, om)

    return jax.shard_map(local, mesh=mesh, in_specs=(spec, spec, spec, P(), P()), out_specs=spec, check_vma=False)
```

```python
import functools

import jax
import jax.numpy as jnp
from jax import lax
from jax.experimental import pallas as pl
from jax.experimental.pallas import tpu as pltpu
from jax.sharding import PartitionSpec as P

MESH = pl.DeviceIdType.MESH
F32 = jnp.float32
DEPTH = 4
ROW0 = 8
LANES = 128
N0, N1, N2, N3 = 10, 6, 8, 8

OFFSETS = [(b, c, a) for a in (-1, 0, 1) for b in (-1, 0, 1) for c in (-1, 0, 1) if (a, b, c) != (0, 0, 0)]


def lane_of(shape):
    return lax.broadcasted_iota(jnp.int32, shape, len(shape) - 1)


def repeat(count, body):
    lax.fori_loop(0, count, lambda i, carry: (body(i), carry)[1], 0, unroll=count)


def turn_lanes(v, by):
    return pltpu.roll(v, -by % LANES, v.ndim - 1)


def shift_x(v, c):
    return turn_lanes(v, 2 * c)


def kernel(dims, u_in, f_in, k_in, w_ref, om_ref, out_ref,
           ext, temp, coef, nat, stage, zsend, zrecv, drecv,
           send_sem, recv_sem, here_sem, pair_send, pair_recv):
    n_y, n_z, ny, nz, sweeps, tiles = dims
    s = DEPTH
    half = LANES // 2
    lo, hi = ROW0, ROW0 + nz
    qe = ny + 2 * s
    first = lo - s
    bx = u_in.shape[0]

    core = lax.axis_index("gx")
    gy = lax.axis_index("gy")
    gz = lax.axis_index("gz")
    zhi, zlo = lax.rem(gz + 1, n_z), lax.rem(gz + n_z - 1, n_z)
    other = 1 - core
    yhi = lax.rem(gy + core, n_y)
    ylo = lax.rem(gy + n_y - other, n_y)

    neighbours = [
        {"gx": other, "gy": yhi, "gz": zhi}, {"gx": other, "gy": ylo, "gz": zhi},
        {"gx": other, "gy": yhi, "gz": zlo}, {"gx": other, "gy": ylo, "gz": zlo},
        {"gz": zhi}, {"gz": zlo}, {"gx": other, "gy": yhi}, {"gx": other, "gy": ylo},
    ]

    barrier = pltpu.get_barrier_semaphore()
    for nb in neighbours:
        pl.semaphore_signal(barrier, inc=1, device_id=nb, device_id_type=MESH)

    mine = pl.multiple_of(core * ny, ny)
    theirs = pl.multiple_of(other * ny, ny)
    my_x = pl.ds(core * bx, bx)
    kap, frc = 2, 3
    fields = (u_in, k_in, f_in)
    kept = [pltpu.make_async_copy(src.at[:, pl.ds(mine, ny)], nat.at[i, my_x], here_sem.at[i])
            for i, src in enumerate(fields)]
    given = [pltpu.make_async_remote_copy(
        src_ref=src.at[:, pl.ds(theirs, ny)], dst_ref=nat.at[i, my_x], send_sem=pair_send.at[i],
        recv_sem=pair_recv.at[i], device_id={"gx": other}, device_id_type=MESH)
        for i, src in enumerate(fields)]
    for i in (1, 2, 0):
        kept[i].start()

    hq = ny // 2

    def copies(arr, slot):
        pieces = [
            (zsend.at[slot, 0, pl.ds((hq - s) * s, s * s)], drecv.at[slot, 0]),
            (zsend.at[slot, 0, pl.ds(0, s * s)], drecv.at[slot, 1]),
            (zsend.at[slot, 1, pl.ds((hq - s) * s, s * s)], drecv.at[slot, 2]),
            (zsend.at[slot, 1, pl.ds(0, s * s)], drecv.at[slot, 3]),
            (zsend.at[slot, 0], zrecv.at[slot, 0]),
            (zsend.at[slot, 1], zrecv.at[slot, 1]),
            (ext.at[arr, pl.ds(ny, s), pl.ds(lo, nz)], ext.at[arr, pl.ds(0, s), pl.ds(lo, nz)]),
            (ext.at[arr, pl.ds(s, s), pl.ds(lo, nz)], ext.at[arr, pl.ds(ny + s, s), pl.ds(lo, nz)]),
        ]
        return [
            pltpu.make_async_remote_copy(
                src_ref=src, dst_ref=dst, send_sem=send_sem.at[slot, i], recv_sem=recv_sem.at[slot, i],
                device_id=neighbours[i], device_id_type=MESH)
            for i, (src, dst) in enumerate(pieces)
        ]

    left = lane_of((s, LANES)) % 2 == 0

    def swap(v):
        return jnp.where(left, turn_lanes(v, 1), turn_lanes(v, -1))

    def begin(arr, slot):
        def pack(q):
            top = jnp.where(left, swap(ext[arr, s + q, pl.ds(hi - s, s)]), ext[arr, s + q + hq, pl.ds(hi - s, s)])
            zsend[slot, 0, pl.ds(q * s, s)] = top
            bottom = jnp.where(left, ext[arr, s + q, pl.ds(lo, s)], swap(ext[arr, s + q + hq, pl.ds(lo, s)]))
            zsend[slot, 1, pl.ds(q * s, s)] = bottom

        repeat(hq, pack)
        for cp in copies(arr, slot):
            cp.start()

    def finish(arr, slot):
        for cp in copies(arr, slot):
            cp.wait()
        def fill(q, low, high):
            ext[arr, q, pl.ds(lo - s, s)] = jnp.where(left, low, swap(ext[arr, q, pl.ds(hi - s, s)]))
            ext[arr, q, pl.ds(hi, s)] = jnp.where(left, swap(ext[arr, q, pl.ds(lo, s)]), high)

        def at(ref, i, q):
            return ref[slot, i, pl.ds(q * s, s)]

        repeat(s, lambda q: fill(q, swap(at(drecv, 0, q)), at(drecv, 2, q)))
        repeat(hq, lambda q: fill(s + q, at(zrecv, 0, q), swap(at(zrecv, 1, q))))
        repeat(hq, lambda q: fill(s + hq + q, swap(at(zrecv, 0, q)), at(zrecv, 1, q)))
        repeat(s, lambda q: fill(s + ny + q, at(drecv, 1, q), swap(at(drecv, 3, q))))

    pl.semaphore_wait(barrier, len(neighbours))
    for i in (1, 2, 0):
        given[i].start()

    @pl.loop(0, 3)
    def _(turn):
        i = lax.rem(turn + 1, 3)
        arr = i + lax.div(i + 1, 2)
        pltpu.make_async_copy(u_in.at[:, pl.ds(mine, ny)], nat.at[i, my_x], here_sem.at[i]).wait()
        pltpu.make_async_remote_copy(
            src_ref=u_in.at[:, pl.ds(theirs, ny)], dst_ref=nat.at[i, my_x], send_sem=pair_send.at[i],
            recv_sem=pair_recv.at[i], device_id={"gx": other}, device_id_type=MESH).wait()

        @pl.loop(0, ny // 8)
        def _(yt):
            y0 = pl.multiple_of(yt * 8, 8)
            planes = jnp.swapaxes(nat[i, :, pl.ds(y0, 8), :], 0, 1)
            for y in range(8):
                stage[y, pl.ds(0, half, stride=2), pl.ds(0, nz)] = planes[y][:, :nz]
                stage[y, pl.ds(1, half, stride=2), pl.ds(0, nz)] = planes[y][:, nz:]
                ext[arr, s + y0 + y, pl.ds(lo, nz)] = stage[y, :, pl.ds(0, nz)].T

        begin(arr, arr)

    every = tuple(range(tiles))
    inner = tuple(t for t in every if first + 8 * t > lo and first + 8 * t + 8 < hi)
    outer = tuple(t for t in every if t not in inner)
    half_w = [0.5 * w_ref[m] for m in range(len(OFFSETS))]
    w_sum = functools.reduce(lambda x, y: x + y, half_w)

    def coefficients(which, q_lo, n, trips, stride):
        @pl.loop(0, trips)
        def _(trip):
            q0 = q_lo + trip * stride
            for t in which:
                base = first + 8 * t
                rows = {b: ext[kap, pl.ds(q0 - 1, n + 2), pl.ds(base + b, 8)] for b in (-1, 0, 1)}
                near = {(a, b): rows[b][1 + a:1 + a + n] for a in (-1, 0, 1) for b in (-1, 0, 1)}
                mid = near[0, 0]
                sums = {0: w_sum * mid}
                for m, (a, b, c) in enumerate(OFFSETS):
                    d = half_w[m] * near[a, b]
                    sums[c] = d if c not in sums else sums[c] + d
                inv = 1.0 / (sums[0] + shift_x(sums[1], 1) + shift_x(sums[-1], -1))
                mids = {0: mid, 1: shift_x(mid, -1), -1: shift_x(mid, 1)}
                invs = {0: inv, 1: shift_x(inv, -1), -1: shift_x(inv, 1)}
                for m, (a, b, c) in enumerate(OFFSETS):
                    coef[pl.ds(q0 - 1, n), t, m] = half_w[m] * (mids[c] + near[a, b]) * invs[c]
                coef[pl.ds(q0 - 1, n), t, len(OFFSETS)] = ext[frc, pl.ds(q0, n), pl.ds(base, 8)] * inv

    CN = 2
    coefficients(inner, s + 1, CN, (ny - 2) // CN, CN)

    @pl.loop(kap, frc + 1)
    def _(arr):
        finish(arr, arr)

    coefficients(outer, s + 1, CN, (ny - 2) // CN, CN)
    coefficients(every, 1, s, 2, qe - 2 - s)

    def update(src, dst, relax, which, q_lo, n, trips, stride=None):
        @pl.loop(0, trips)
        def _(trip):
            q0 = q_lo + trip * (stride or n)
            for t in which:
                base = first + 8 * t
                rows = {b: src[pl.ds(q0 - 1, n + 2), pl.ds(base + b, 8)] for b in (-1, 0, 1)}
                sums = {0: coef[pl.ds(q0 - 1, n), t, len(OFFSETS)]}
                for m, (a, b, c) in enumerate(OFFSETS):
                    p = coef[pl.ds(q0 - 1, n), t, m] * rows[b][1 + a:1 + a + n]
                    sums[c] = p if c not in sums else sums[c] + p
                total = sums[0] + shift_x(sums[1], 1) + shift_x(sums[-1], -1)
                mid = rows[0][1:1 + n]
                dst[pl.ds(q0, n), pl.ds(base, 8)] = mid + relax * (total - mid)

    def group(slot, k0, send):
        arr, nxt = ext.at[slot], ext.at[1 - slot]
        bufs = [arr, temp]
        relax = om_ref[k0]
        update(arr, temp, relax, inner, s + 1, N0, (ny - 2) // N0)
        finish(slot, slot)
        update(arr, temp, relax, outer, s + 1, N0, (ny - 2) // N0)
        update(arr, temp, relax, every, 1, s, 2, qe - 2 - s)
        for j in range(1, s - 1):
            rows_now = qe - 2 - 2 * j
            update(bufs[j % 2], bufs[(j + 1) % 2], om_ref[k0 + j], every, 1 + j, N1, -(-rows_now // N1))
        src, relax = bufs[(s - 1) % 2], om_ref[k0 + s - 1]
        update(src, nxt, relax, every, s, s, 2, ny - s)
        update(src, nxt, relax, outer, 2 * s, N2, (ny - 2 * s) // N2)
        send()
        update(src, nxt, relax, inner, 2 * s, N3, (ny - 2 * s) // N3)

    groups = sweeps // s

    @pl.loop(0, groups)
    def _(i):
        slot = lax.rem(i, 2)

        def send():
            @pl.when(i < groups - 1)
            def _():
                begin(1 - slot, 1 - slot)

        group(slot, s * i, send)

    last = groups % 2

    def home(yt):
        rows = pl.ds(pl.multiple_of(core * ny + yt * 8, 8), 8)
        return (pltpu.make_async_copy(
                    nat.at[0, my_x, pl.ds(pl.multiple_of(yt * 8, 8), 8)], out_ref.at[:, rows], here_sem.at[yt]),
                pltpu.make_async_remote_copy(
                    src_ref=nat.at[0, pl.ds(other * bx, bx), pl.ds(pl.multiple_of(yt * 8, 8), 8)], dst_ref=out_ref.at[:, rows],
                    send_sem=pair_send.at[yt], recv_sem=pair_recv.at[yt], device_id={"gx": other},
                    device_id_type=MESH))

    @pl.loop(0, ny // 8)
    def _(step):
        yt = pl.multiple_of(step * 8, 8)
        planes = []
        for y in range(8):
            stage[y, :, pl.ds(0, nz)] = ext[last, s + yt + y, pl.ds(lo, nz)].T
            planes.append(jnp.concatenate([stage[y, pl.ds(0, half, stride=2), pl.ds(0, nz)],
                                           stage[y, pl.ds(1, half, stride=2), pl.ds(0, nz)]], axis=1))
        nat[0, :, pl.ds(yt, 8), :] = jnp.swapaxes(jnp.stack(planes), 0, 1)
        for cp in home(step):
            cp.start()

    @pl.loop(0, ny // 8)
    def _(step):
        for cp in home(step):
            cp.wait()


def solution(mesh):
    spec = P(("batch", "gx"), "gy", "gz")
    n_x, n_y, n_z = mesh.shape["gx"], mesh.shape["gy"], mesh.shape["gz"]

    def local(u, f, k, w, om):
        bx, by, bz = u.shape
        ny, nz = by // n_x, bz // 2
        s = DEPTH
        tiles = -(-(nz + 2 * s - 1) // 8)
        rows = ROW0 + -(-(nz + s) // 8) * 8
        qe = ny + 2 * s
        hbm = pl.BlockSpec(memory_space=pl.ANY)
        sm = pl.BlockSpec(memory_space=pltpu.SMEM)
        dma = pltpu.SemaphoreType.DMA
        return pl.pallas_call(
            functools.partial(kernel, (n_y, n_z, ny, nz, om.shape[0], tiles)),
            out_shape=jax.ShapeDtypeStruct(u.shape, F32),
            in_specs=[hbm, hbm, hbm, sm, sm],
            out_specs=hbm,
            scratch_shapes=[
                pltpu.VMEM((4, qe, rows, LANES), F32),
                pltpu.VMEM((qe, rows, LANES), F32),
                pltpu.VMEM((qe - 2, tiles, len(OFFSETS) + 2, 8, LANES), F32),
                pltpu.VMEM((3, n_x * bx, ny, bz), F32),
                pltpu.VMEM((8, LANES, LANES), F32),
                pltpu.VMEM((4, 2, ny // 2 * s, LANES), F32),
                pltpu.VMEM((4, 2, ny // 2 * s, LANES), F32),
                pltpu.VMEM((4, 4, s * s, LANES), F32),
                dma((4, 8)), dma((4, 8)), dma((4,)), dma((4,)), dma((4,)),
            ],
            compiler_params=pltpu.CompilerParams(collective_id=0, has_side_effects=True, vmem_limit_bytes=56 << 20),
        )(u, f, k, w, om)

    return jax.shard_map(local, mesh=mesh, in_specs=(spec, spec, spec, P(), P()), out_specs=spec, check_vma=False)
```

```python
import functools

import jax
import jax.numpy as jnp
from jax import lax
from jax.experimental import pallas as pl
from jax.experimental.pallas import tpu as pltpu
from jax.sharding import PartitionSpec as P

MESH = pl.DeviceIdType.MESH
F32 = jnp.float32
DEPTH = 4
ROW0 = 8
LANES = 128
N0, N1, N2, N3, N4 = 10, 12, 16, 12, 15

OFFSETS = [(b, c, a) for a in (-1, 0, 1) for b in (-1, 0, 1) for c in (-1, 0, 1) if (a, b, c) != (0, 0, 0)]


def lane_of(shape):
    return lax.broadcasted_iota(jnp.int32, shape, len(shape) - 1)


def repeat(count, body):
    lax.fori_loop(0, count, lambda i, carry: (body(i), carry)[1], 0, unroll=count)


def turn_lanes(v, by):
    return pltpu.roll(v, -by % LANES, v.ndim - 1)


def shift_x(v, c):
    return turn_lanes(v, 2 * c)


def kernel(dims, u_in, f_in, k_in, w_ref, om_ref, out_ref,
           ext, temp, coef, nat, stage, zsend, zrecv, dsend, drecv,
           send_sem, recv_sem, here_sem, pair_send, pair_recv):
    n_y, n_z, ny, nz, sweeps, tiles = dims
    s = DEPTH
    half = LANES // 2
    lo, hi = ROW0, ROW0 + nz
    qe = ny + 2 * s
    first = lo - s
    bx = u_in.shape[0]

    core = lax.axis_index("gx")
    gy = lax.axis_index("gy")
    gz = lax.axis_index("gz")
    zhi, zlo = lax.rem(gz + 1, n_z), lax.rem(gz + n_z - 1, n_z)
    other = 1 - core
    yhi = lax.rem(gy + core, n_y)
    ylo = lax.rem(gy + n_y - other, n_y)

    neighbours = [
        {"gx": other, "gy": yhi, "gz": zhi}, {"gx": other, "gy": ylo, "gz": zhi},
        {"gx": other, "gy": yhi, "gz": zlo}, {"gx": other, "gy": ylo, "gz": zlo},
        {"gz": zhi}, {"gz": zlo}, {"gx": other, "gy": yhi}, {"gx": other, "gy": ylo},
    ]

    barrier = pltpu.get_barrier_semaphore()
    for nb in neighbours:
        pl.semaphore_signal(barrier, inc=1, device_id=nb, device_id_type=MESH)

    mine = pl.multiple_of(core * ny, ny)
    theirs = pl.multiple_of(other * ny, ny)
    my_x = pl.ds(core * bx, bx)
    kap, frc = 2, 3
    fields = (u_in, k_in, f_in)
    kept = [pltpu.make_async_copy(src.at[:, pl.ds(mine, ny)], nat.at[i, my_x], here_sem.at[i])
            for i, src in enumerate(fields)]
    given = [pltpu.make_async_remote_copy(
        src_ref=src.at[:, pl.ds(theirs, ny)], dst_ref=nat.at[i, my_x], send_sem=pair_send.at[i],
        recv_sem=pair_recv.at[i], device_id={"gx": other}, device_id_type=MESH)
        for i, src in enumerate(fields)]
    for i in (1, 2, 0):
        kept[i].start()

    hq = ny // 2

    def copies(arr, slot, which):
        pieces = [(dsend.at[slot, i], drecv.at[slot, i]) for i in range(4)] + [
            (zsend.at[slot, 0], zrecv.at[slot, 0]),
            (zsend.at[slot, 1], zrecv.at[slot, 1]),
            (ext.at[arr, pl.ds(ny, s), pl.ds(lo, nz)], ext.at[arr, pl.ds(0, s), pl.ds(lo, nz)]),
            (ext.at[arr, pl.ds(s, s), pl.ds(lo, nz)], ext.at[arr, pl.ds(ny + s, s), pl.ds(lo, nz)]),
        ]
        return [
            pltpu.make_async_remote_copy(
                src_ref=pieces[i][0], dst_ref=pieces[i][1], send_sem=send_sem.at[slot, i],
                recv_sem=recv_sem.at[slot, i], device_id=neighbours[i], device_id_type=MESH)
            for i in which
        ]

    CORNERS, Z_FACES, Y_FACES = (0, 1, 2, 3), (4, 5), (6, 7)
    left = lane_of((s, LANES)) % 2 == 0
    below, bottom, top, above = (pl.ds(row, s) for row in (lo - s, lo, hi - s, hi))

    def swap(v):
        return jnp.where(left, turn_lanes(v, 1), turn_lanes(v, -1))

    def part(q):
        return pl.ds(q * s, s)

    def begin_z(arr, slot):
        def corner(q):
            for i, (q0, rows) in enumerate(((ny, top), (s, top), (ny, bottom), (s, bottom))):
                dsend[slot, i, part(q)] = swap(ext[arr, q0 + q, rows])

        def pack(q):
            zsend[slot, 0, part(q)] = jnp.where(
                left, swap(ext[arr, s + q, top]), ext[arr, s + q + hq, top])
            zsend[slot, 1, part(q)] = jnp.where(
                left, ext[arr, s + q, bottom], swap(ext[arr, s + q + hq, bottom]))

        repeat(hq, pack)
        for cp in copies(arr, slot, Z_FACES):
            cp.start()
        repeat(s, corner)
        for cp in copies(arr, slot, CORNERS):
            cp.start()

    def begin_y(arr, slot):
        for cp in copies(arr, slot, Y_FACES):
            cp.start()

        def local(q):
            ext[arr, s + q, below] = swap(ext[arr, s + q, top])
            ext[arr, s + q, above] = swap(ext[arr, s + q, bottom])

        repeat(ny, local)

    def finish_z(arr, slot):
        for cp in copies(arr, slot, Z_FACES):
            cp.wait()

        def fill(q):
            low, high = zrecv[slot, 0, part(q)], zrecv[slot, 1, part(q)]
            ext[arr, s + q, below] = jnp.where(left, low, ext[arr, s + q, below])
            ext[arr, s + q, above] = jnp.where(left, ext[arr, s + q, above], swap(high))
            ext[arr, s + q + hq, below] = jnp.where(left, swap(low), ext[arr, s + q + hq, below])
            ext[arr, s + q + hq, above] = jnp.where(left, ext[arr, s + q + hq, above], high)

        repeat(hq, fill)

    def finish_y(arr, slot):
        for cp in copies(arr, slot, CORNERS + Y_FACES):
            cp.wait()

        def fill(q):
            for i, q0 in ((0, 0), (1, s + ny)):
                ext[arr, q0 + q, below] = jnp.where(left, drecv[slot, i, part(q)], swap(ext[arr, q0 + q, top]))
                ext[arr, q0 + q, above] = jnp.where(left, swap(ext[arr, q0 + q, bottom]), drecv[slot, i + 2, part(q)])

        repeat(s, fill)

    pl.semaphore_wait(barrier, len(neighbours))
    for i in (1, 2, 0):
        given[i].start()

    @pl.loop(0, 3)
    def _(turn):
        i = lax.rem(turn + 1, 3)
        arr = i + lax.div(i + 1, 2)
        pltpu.make_async_copy(u_in.at[:, pl.ds(mine, ny)], nat.at[i, my_x], here_sem.at[i]).wait()
        pltpu.make_async_remote_copy(
            src_ref=u_in.at[:, pl.ds(theirs, ny)], dst_ref=nat.at[i, my_x], send_sem=pair_send.at[i],
            recv_sem=pair_recv.at[i], device_id={"gx": other}, device_id_type=MESH).wait()

        @pl.loop(0, ny // 8)
        def _(yt):
            y0 = pl.multiple_of(yt * 8, 8)
            planes = jnp.swapaxes(nat[i, :, pl.ds(y0, 8), :], 0, 1)
            for y in range(8):
                stage[y, pl.ds(0, half, stride=2), pl.ds(0, nz)] = planes[y][:, :nz]
                stage[y, pl.ds(1, half, stride=2), pl.ds(0, nz)] = planes[y][:, nz:]
                ext[arr, s + y0 + y, pl.ds(lo, nz)] = stage[y, :, pl.ds(0, nz)].T

        begin_z(arr, arr)
        begin_y(arr, arr)

    every = tuple(range(tiles))
    inner = tuple(t for t in every if first + 8 * t > lo and first + 8 * t + 8 < hi)
    outer = tuple(t for t in every if t not in inner)
    half_w = [0.5 * w_ref[m] for m in range(len(OFFSETS))]
    w_sum = functools.reduce(lambda x, y: x + y, half_w)

    def coefficients(which, q_lo, n, trips, stride):
        @pl.loop(0, trips)
        def _(trip):
            q0 = q_lo + trip * stride
            for t in which:
                base = first + 8 * t
                rows = {b: ext[kap, pl.ds(q0 - 1, n + 2), pl.ds(base + b, 8)] for b in (-1, 0, 1)}
                near = {(a, b): rows[b][1 + a:1 + a + n] for a in (-1, 0, 1) for b in (-1, 0, 1)}
                mid = near[0, 0]
                sums = {0: w_sum * mid}
                for m, (a, b, c) in enumerate(OFFSETS):
                    d = half_w[m] * near[a, b]
                    sums[c] = d if c not in sums else sums[c] + d
                inv = 1.0 / (sums[0] + shift_x(sums[1], 1) + shift_x(sums[-1], -1))
                mids = {0: mid, 1: shift_x(mid, -1), -1: shift_x(mid, 1)}
                invs = {0: inv, 1: shift_x(inv, -1), -1: shift_x(inv, 1)}
                for m, (a, b, c) in enumerate(OFFSETS):
                    coef[pl.ds(q0 - 1, n), t, m] = half_w[m] * (mids[c] + near[a, b]) * invs[c]
                coef[pl.ds(q0 - 1, n), t, len(OFFSETS)] = ext[frc, pl.ds(q0, n), pl.ds(base, 8)] * inv

    CN = 5
    coefficients(inner, s + 1, CN, (ny - 2) // CN, CN)

    @pl.loop(kap, frc + 1)
    def _(arr):
        finish_z(arr, arr)
        finish_y(arr, arr)

    coefficients(outer, s + 1, CN, (ny - 2) // CN, CN)
    coefficients(every, 1, s, 2, qe - 2 - s)

    def update(src, dst, relax, which, q_lo, n, trips, stride=None):
        @pl.loop(0, trips)
        def _(trip):
            q0 = q_lo + trip * (stride or n)
            for t in which:
                base = first + 8 * t
                rows = {b: src[pl.ds(q0 - 1, n + 2), pl.ds(base + b, 8)] for b in (-1, 0, 1)}
                sums = {0: coef[pl.ds(q0 - 1, n), t, len(OFFSETS)]}
                for m, (a, b, c) in enumerate(OFFSETS):
                    p = coef[pl.ds(q0 - 1, n), t, m] * rows[b][1 + a:1 + a + n]
                    sums[c] = p if c not in sums else sums[c] + p
                total = sums[0] + shift_x(sums[1], 1) + shift_x(sums[-1], -1)
                mid = rows[0][1:1 + n]
                dst[pl.ds(q0, n), pl.ds(base, 8)] = mid + relax * (total - mid)

    groups = sweeps // s

    @pl.loop(0, groups)
    def _(i):
        slot = lax.rem(i, 2)
        arr, nxt = ext.at[slot], ext.at[1 - slot]
        bufs = [arr, temp]
        relax = om_ref[s * i]
        update(arr, temp, relax, inner, s + 1, N0, (ny - 2) // N0)
        finish_z(slot, slot)
        update(arr, temp, relax, outer, s + 1, N4, (ny - 2) // N4)
        finish_y(slot, slot)
        update(arr, temp, relax, every, 1, s, 2, qe - 2 - s)
        for j in range(1, s - 1):
            rows_now = qe - 2 - 2 * j
            update(bufs[j % 2], bufs[(j + 1) % 2], om_ref[s * i + j], every, 1 + j, N1, -(-rows_now // N1))
        src, relax = bufs[(s - 1) % 2], om_ref[s * i + s - 1]
        update(src, nxt, relax, outer, s, N2, ny // N2)

        @pl.when(i < groups - 1)
        def _():
            begin_z(1 - slot, 1 - slot)

        update(src, nxt, relax, inner, s, s, 2, ny - s)

        @pl.when(i < groups - 1)
        def _():
            begin_y(1 - slot, 1 - slot)

        update(src, nxt, relax, inner, 2 * s, N3, (ny - 2 * s) // N3)

    last = groups % 2

    def home(yt):
        rows = pl.ds(pl.multiple_of(core * ny + yt * 8, 8), 8)
        return (pltpu.make_async_copy(
                    nat.at[0, my_x, pl.ds(pl.multiple_of(yt * 8, 8), 8)], out_ref.at[:, rows], here_sem.at[yt]),
                pltpu.make_async_remote_copy(
                    src_ref=nat.at[0, pl.ds(other * bx, bx), pl.ds(pl.multiple_of(yt * 8, 8), 8)], dst_ref=out_ref.at[:, rows],
                    send_sem=pair_send.at[yt], recv_sem=pair_recv.at[yt], device_id={"gx": other},
                    device_id_type=MESH))

    @pl.loop(0, ny // 8)
    def _(step):
        yt = pl.multiple_of(step * 8, 8)
        planes = []
        for y in range(8):
            stage[y, :, pl.ds(0, nz)] = ext[last, s + yt + y, pl.ds(lo, nz)].T
            planes.append(jnp.concatenate([stage[y, pl.ds(0, half, stride=2), pl.ds(0, nz)],
                                           stage[y, pl.ds(1, half, stride=2), pl.ds(0, nz)]], axis=1))
        nat[0, :, pl.ds(yt, 8), :] = jnp.swapaxes(jnp.stack(planes), 0, 1)
        for cp in home(step):
            cp.start()

    @pl.loop(0, ny // 8)
    def _(step):
        for cp in home(step):
            cp.wait()


def solution(mesh):
    spec = P(("batch", "gx"), "gy", "gz")
    n_x, n_y, n_z = mesh.shape["gx"], mesh.shape["gy"], mesh.shape["gz"]

    def local(u, f, k, w, om):
        bx, by, bz = u.shape
        ny, nz = by // n_x, bz // 2
        s = DEPTH
        tiles = -(-(nz + 2 * s - 1) // 8)
        rows = ROW0 + -(-(nz + s) // 8) * 8
        qe = ny + 2 * s
        hbm = pl.BlockSpec(memory_space=pl.ANY)
        sm = pl.BlockSpec(memory_space=pltpu.SMEM)
        dma = pltpu.SemaphoreType.DMA
        return pl.pallas_call(
            functools.partial(kernel, (n_y, n_z, ny, nz, om.shape[0], tiles)),
            out_shape=jax.ShapeDtypeStruct(u.shape, F32),
            in_specs=[hbm, hbm, hbm, sm, sm],
            out_specs=hbm,
            scratch_shapes=[
                pltpu.VMEM((4, qe, rows, LANES), F32),
                pltpu.VMEM((qe, rows, LANES), F32),
                pltpu.VMEM((qe - 2, tiles, len(OFFSETS) + 2, 8, LANES), F32),
                pltpu.VMEM((3, n_x * bx, ny, bz), F32),
                pltpu.VMEM((8, LANES, LANES), F32),
                pltpu.VMEM((4, 2, ny // 2 * s, LANES), F32),
                pltpu.VMEM((4, 2, ny // 2 * s, LANES), F32),
                pltpu.VMEM((4, 4, s * s, LANES), F32),
                pltpu.VMEM((4, 4, s * s, LANES), F32),
                dma((4, 8)), dma((4, 8)), dma((4,)), dma((4,)), dma((4,)),
            ],
            compiler_params=pltpu.CompilerParams(collective_id=0, has_side_effects=True, vmem_limit_bytes=56 << 20),
        )(u, f, k, w, om)

    return jax.shard_map(local, mesh=mesh, in_specs=(spec, spec, spec, P(), P()), out_specs=spec, check_vma=False)
```

```python
import functools

import jax
import jax.numpy as jnp
from jax import lax
from jax.experimental import pallas as pl
from jax.experimental.pallas import tpu as pltpu
from jax.sharding import PartitionSpec as P

MESH = pl.DeviceIdType.MESH
F32 = jnp.float32
DEPTH = 4
ROW0 = 8
LANES = 128
N0, N1, N2, N3, N4 = 10, 18, 16, 24, 30

OFFSETS = [(b, c, a) for a in (-1, 0, 1) for b in (-1, 0, 1) for c in (-1, 0, 1) if (a, b, c) != (0, 0, 0)]


def lane_of(shape):
    return lax.broadcasted_iota(jnp.int32, shape, len(shape) - 1)


def repeat(count, body):
    lax.fori_loop(0, count, lambda i, carry: (body(i), carry)[1], 0, unroll=count)


def turn_lanes(v, by):
    return pltpu.roll(v, -by % LANES, v.ndim - 1)


def shift_x(v, c):
    return turn_lanes(v, 2 * c)


def kernel(dims, u_in, f_in, k_in, w_in, om_in, out_ref,
           ext, temp, coef, nat, stage, zsend, zrecv, dsend, drecv,
           send_sem, recv_sem, here_sem, pair_send, pair_recv, w_ref, om_ref, scalar_sem):
    n_y, n_z, ny, nz, sweeps, tiles = dims
    s = DEPTH
    half = LANES // 2
    lo, hi = ROW0, ROW0 + nz
    qe = ny + 2 * s
    first = lo - s
    bx = u_in.shape[0]

    core = lax.axis_index("gx")
    gy = lax.axis_index("gy")
    gz = lax.axis_index("gz")
    zhi, zlo = lax.rem(gz + 1, n_z), lax.rem(gz + n_z - 1, n_z)
    other = 1 - core
    yhi = lax.rem(gy + core, n_y)
    ylo = lax.rem(gy + n_y - other, n_y)

    neighbours = [
        {"gx": other, "gy": yhi, "gz": zhi}, {"gx": other, "gy": ylo, "gz": zhi},
        {"gx": other, "gy": yhi, "gz": zlo}, {"gx": other, "gy": ylo, "gz": zlo},
        {"gz": zhi}, {"gz": zlo}, {"gx": other, "gy": yhi}, {"gx": other, "gy": ylo},
    ]

    barrier = pltpu.get_barrier_semaphore()
    for nb in neighbours:
        pl.semaphore_signal(barrier, inc=1, device_id=nb, device_id_type=MESH)

    mine = pl.multiple_of(core * ny, ny)
    theirs = pl.multiple_of(other * ny, ny)
    my_x = pl.ds(core * bx, bx)
    kap, frc = 2, 3
    fields = (u_in, k_in, f_in)
    kept = [pltpu.make_async_copy(src.at[:, pl.ds(mine, ny)], nat.at[i, my_x], here_sem.at[i])
            for i, src in enumerate(fields)]

    def give(i, yt):
        return pltpu.make_async_remote_copy(
            src_ref=fields[i].at[:, pl.ds(pl.multiple_of(theirs + yt * 8, 8), 8)],
            dst_ref=nat.at[i, my_x, pl.ds(pl.multiple_of(yt * 8, 8), 8)], send_sem=pair_send.at[i, yt],
            recv_sem=pair_recv.at[i, yt], device_id={"gx": other}, device_id_type=MESH)

    for i in (1, 2, 0):
        kept[i].start()
    scalars = [pltpu.make_async_copy(w_in, w_ref, scalar_sem.at[0]), pltpu.make_async_copy(om_in, om_ref, scalar_sem.at[1])]
    for cp in scalars:
        cp.start()

    hq = ny // 2

    def copies(arr, slot, which):
        pieces = [(dsend.at[slot, i], drecv.at[slot, i]) for i in range(4)] + [
            (zsend.at[slot, 0], zrecv.at[slot, 0]),
            (zsend.at[slot, 1], zrecv.at[slot, 1]),
            (ext.at[arr, pl.ds(ny, s), pl.ds(lo, nz)], ext.at[arr, pl.ds(0, s), pl.ds(lo, nz)]),
            (ext.at[arr, pl.ds(s, s), pl.ds(lo, nz)], ext.at[arr, pl.ds(ny + s, s), pl.ds(lo, nz)]),
        ]
        return [
            pltpu.make_async_remote_copy(
                src_ref=pieces[i][0], dst_ref=pieces[i][1], send_sem=send_sem.at[slot, i],
                recv_sem=recv_sem.at[slot, i], device_id=neighbours[i], device_id_type=MESH)
            for i in which
        ]

    CORNERS, Z_FACES, Y_FACES = (0, 1, 2, 3), (4, 5), (6, 7)
    left = lane_of((s, LANES)) % 2 == 0
    below, bottom, top, above = (pl.ds(row, s) for row in (lo - s, lo, hi - s, hi))

    def swap(v):
        return jnp.where(left, turn_lanes(v, 1), turn_lanes(v, -1))

    def part(q):
        return pl.ds(q * s, s)

    def begin_z(arr, slot):
        def corner(q):
            for i, (q0, rows) in enumerate(((ny, top), (s, top), (ny, bottom), (s, bottom))):
                dsend[slot, i, part(q)] = swap(ext[arr, q0 + q, rows])

        def pack(q):
            zsend[slot, 0, part(q)] = jnp.where(
                left, swap(ext[arr, s + q, top]), ext[arr, s + q + hq, top])
            zsend[slot, 1, part(q)] = jnp.where(
                left, ext[arr, s + q, bottom], swap(ext[arr, s + q + hq, bottom]))

        repeat(hq, pack)
        for cp in copies(arr, slot, Z_FACES):
            cp.start()
        repeat(s, corner)
        for cp in copies(arr, slot, CORNERS):
            cp.start()

    def begin_y(arr, slot):
        for cp in copies(arr, slot, Y_FACES):
            cp.start()

        def local(q):
            ext[arr, s + q, below] = swap(ext[arr, s + q, top])
            ext[arr, s + q, above] = swap(ext[arr, s + q, bottom])

        repeat(ny, local)

    def finish_z(arr, slot):
        for cp in copies(arr, slot, Z_FACES):
            cp.wait()

        def fill(q):
            low, high = zrecv[slot, 0, part(q)], zrecv[slot, 1, part(q)]
            ext[arr, s + q, below] = jnp.where(left, low, ext[arr, s + q, below])
            ext[arr, s + q, above] = jnp.where(left, ext[arr, s + q, above], swap(high))
            ext[arr, s + q + hq, below] = jnp.where(left, swap(low), ext[arr, s + q + hq, below])
            ext[arr, s + q + hq, above] = jnp.where(left, ext[arr, s + q + hq, above], high)

        repeat(hq, fill)

    def finish_y(arr, slot):
        for cp in copies(arr, slot, CORNERS + Y_FACES):
            cp.wait()

        def fill(q):
            for i, q0 in ((0, 0), (1, s + ny)):
                ext[arr, q0 + q, below] = jnp.where(left, drecv[slot, i, part(q)], swap(ext[arr, q0 + q, top]))
                ext[arr, q0 + q, above] = jnp.where(left, swap(ext[arr, q0 + q, bottom]), drecv[slot, i + 2, part(q)])

        repeat(s, fill)

    pl.semaphore_wait(barrier, len(neighbours))
    for i in (1, 2, 0):
        for yt in range(ny // 8):
            give(i, yt).start()

    @pl.loop(0, 3)
    def _(turn):
        i = lax.rem(turn + 1, 3)
        arr = i + lax.div(i + 1, 2)
        pltpu.make_async_copy(u_in.at[:, pl.ds(mine, ny)], nat.at[i, my_x], here_sem.at[i]).wait()
        @pl.loop(0, ny // 8)
        def _(yt):
            pltpu.make_async_remote_copy(
                src_ref=u_in.at[:, pl.ds(0, 8)], dst_ref=nat.at[i, my_x, pl.ds(pl.multiple_of(yt * 8, 8), 8)],
                send_sem=pair_send.at[i, yt], recv_sem=pair_recv.at[i, yt], device_id={"gx": other},
                device_id_type=MESH).wait()
            y0 = pl.multiple_of(yt * 8, 8)
            planes = jnp.swapaxes(nat[i, :, pl.ds(y0, 8), :], 0, 1)
            for y in range(8):
                stage[y, pl.ds(0, half, stride=2), pl.ds(0, nz)] = planes[y][:, :nz]
                stage[y, pl.ds(1, half, stride=2), pl.ds(0, nz)] = planes[y][:, nz:]
                ext[arr, s + y0 + y, pl.ds(lo, nz)] = stage[y, :, pl.ds(0, nz)].T

        begin_z(arr, arr)
        begin_y(arr, arr)

    every = tuple(range(tiles))
    inner = tuple(t for t in every if first + 8 * t > lo and first + 8 * t + 8 < hi)
    outer = tuple(t for t in every if t not in inner)
    for cp in scalars:
        cp.wait()
    half_w = [0.5 * w_ref[m] for m in range(len(OFFSETS))]
    w_sum = functools.reduce(lambda x, y: x + y, half_w)

    def coefficients(which, q_lo, n, trips, stride):
        @pl.loop(0, trips)
        def _(trip):
            q0 = q_lo + trip * stride
            for t in which:
                base = first + 8 * t
                rows = {b: ext[kap, pl.ds(q0 - 1, n + 2), pl.ds(base + b, 8)] for b in (-1, 0, 1)}
                near = {(a, b): rows[b][1 + a:1 + a + n] for a in (-1, 0, 1) for b in (-1, 0, 1)}
                mid = near[0, 0]
                sums = {0: w_sum * mid}
                for m, (a, b, c) in enumerate(OFFSETS):
                    d = half_w[m] * near[a, b]
                    sums[c] = d if c not in sums else sums[c] + d
                inv = 1.0 / (sums[0] + shift_x(sums[1], 1) + shift_x(sums[-1], -1))
                mids = {0: mid, 1: shift_x(mid, -1), -1: shift_x(mid, 1)}
                invs = {0: inv, 1: shift_x(inv, -1), -1: shift_x(inv, 1)}
                for m, (a, b, c) in enumerate(OFFSETS):
                    coef[pl.ds(q0 - 1, n), t, m] = half_w[m] * (mids[c] + near[a, b]) * invs[c]
                coef[pl.ds(q0 - 1, n), t, len(OFFSETS)] = ext[frc, pl.ds(q0, n), pl.ds(base, 8)] * inv

    CN = 6
    coefficients(inner, s + 1, CN, (ny - 2) // CN, CN)

    def update(src, dst, relax, which, q_lo, n, trips, stride=None):
        @pl.loop(0, trips)
        def _(trip):
            q0 = q_lo + trip * (stride or n)
            for t in which:
                base = first + 8 * t
                rows = {b: src[pl.ds(q0 - 1, n + 2), pl.ds(base + b, 8)] for b in (-1, 0, 1)}
                sums = {0: coef[pl.ds(q0 - 1, n), t, len(OFFSETS)]}
                for m, (a, b, c) in enumerate(OFFSETS):
                    p = coef[pl.ds(q0 - 1, n), t, m] * rows[b][1 + a:1 + a + n]
                    sums[c] = p if c not in sums else sums[c] + p
                total = sums[0] + shift_x(sums[1], 1) + shift_x(sums[-1], -1)
                mid = rows[0][1:1 + n]
                dst[pl.ds(q0, n), pl.ds(base, 8)] = mid + relax * (total - mid)

    groups = sweeps // s

    @pl.loop(0, groups)
    def _(i):
        slot = lax.rem(i, 2)
        arr, nxt = ext.at[slot], ext.at[1 - slot]
        bufs = [arr, temp]
        relax = om_ref[s * i]
        update(arr, temp, relax, inner, s + 1, N0, (ny - 2) // N0)

        @pl.when(i == 0)
        def _():
            @pl.loop(kap, frc + 1)
            def _(field):
                finish_z(field, field)
                finish_y(field, field)

            coefficients(outer, s + 1, CN, (ny - 2) // CN, CN)
            coefficients(every, 1, s, 2, qe - 2 - s)

        finish_z(slot, slot)
        update(arr, temp, relax, outer, s + 1, N4, (ny - 2) // N4)
        finish_y(slot, slot)
        update(arr, temp, relax, every, 1, s, 2, qe - 2 - s)
        for j in range(1, s - 1):
            rows_now = qe - 2 - 2 * j
            update(bufs[j % 2], bufs[(j + 1) % 2], om_ref[s * i + j], every, 1 + j, N1, -(-rows_now // N1))
        src, relax = bufs[(s - 1) % 2], om_ref[s * i + s - 1]
        update(src, nxt, relax, outer, s, N2, ny // N2)

        @pl.when(i < groups - 1)
        def _():
            begin_z(1 - slot, 1 - slot)

        update(src, nxt, relax, inner, s, s, 2, ny - s)

        @pl.when(i < groups - 1)
        def _():
            begin_y(1 - slot, 1 - slot)

        update(src, nxt, relax, inner, 2 * s, N3, (ny - 2 * s) // N3)

    last = groups % 2

    def home(yt):
        rows = pl.ds(pl.multiple_of(core * ny + yt * 8, 8), 8)
        return (pltpu.make_async_copy(
                    nat.at[0, my_x, pl.ds(pl.multiple_of(yt * 8, 8), 8)], out_ref.at[:, rows], here_sem.at[yt]),
                pltpu.make_async_remote_copy(
                    src_ref=nat.at[0, pl.ds(other * bx, bx), pl.ds(pl.multiple_of(yt * 8, 8), 8)], dst_ref=out_ref.at[:, rows],
                    send_sem=pair_send.at[0, yt], recv_sem=pair_recv.at[0, yt], device_id={"gx": other},
                    device_id_type=MESH))

    @pl.loop(0, ny // 8)
    def _(step):
        yt = pl.multiple_of(step * 8, 8)
        planes = []
        for y in range(8):
            stage[y, :, pl.ds(0, nz)] = ext[last, s + yt + y, pl.ds(lo, nz)].T
            planes.append(jnp.concatenate([stage[y, pl.ds(0, half, stride=2), pl.ds(0, nz)],
                                           stage[y, pl.ds(1, half, stride=2), pl.ds(0, nz)]], axis=1))
        nat[0, :, pl.ds(yt, 8), :] = jnp.swapaxes(jnp.stack(planes), 0, 1)
        for cp in home(step):
            cp.start()

    @pl.loop(0, ny // 8)
    def _(step):
        for cp in home(step):
            cp.wait()


def solution(mesh):
    spec = P(("batch", "gx"), "gy", "gz")
    n_x, n_y, n_z = mesh.shape["gx"], mesh.shape["gy"], mesh.shape["gz"]

    def local(u, f, k, w, om):
        bx, by, bz = u.shape
        ny, nz = by // n_x, bz // 2
        s = DEPTH
        tiles = -(-(nz + 2 * s - 1) // 8)
        rows = ROW0 + -(-(nz + s) // 8) * 8
        qe = ny + 2 * s
        hbm = pl.BlockSpec(memory_space=pl.ANY)
        dma = pltpu.SemaphoreType.DMA
        return pl.pallas_call(
            functools.partial(kernel, (n_y, n_z, ny, nz, om.shape[0], tiles)),
            out_shape=jax.ShapeDtypeStruct(u.shape, F32),
            in_specs=[hbm, hbm, hbm, hbm, hbm],
            out_specs=hbm,
            scratch_shapes=[
                pltpu.VMEM((4, qe, rows, LANES), F32),
                pltpu.VMEM((qe, rows, LANES), F32),
                pltpu.VMEM((qe - 2, tiles, len(OFFSETS) + 2, 8, LANES), F32),
                pltpu.VMEM((3, n_x * bx, ny, bz), F32),
                pltpu.VMEM((8, LANES, LANES), F32),
                pltpu.VMEM((4, 2, ny // 2 * s, LANES), F32),
                pltpu.VMEM((4, 2, ny // 2 * s, LANES), F32),
                pltpu.VMEM((4, 4, s * s, LANES), F32),
                pltpu.VMEM((4, 4, s * s, LANES), F32),
                dma((4, 8)), dma((4, 8)), dma((4,)), dma((3, ny // 8)), dma((3, ny // 8)),
                pltpu.SMEM(w.shape, F32), pltpu.SMEM(om.shape, F32), dma((2,)),
            ],
            compiler_params=pltpu.CompilerParams(collective_id=0, has_side_effects=True, vmem_limit_bytes=56 << 20),
        )(u, f, k, w, om)

    return jax.shard_map(local, mesh=mesh, in_specs=(spec, spec, spec, P(), P()), out_specs=spec, check_vma=False)
```

```python
import functools

import jax
import jax.numpy as jnp
from jax import lax
from jax.experimental import pallas as pl
from jax.experimental.pallas import tpu as pltpu
from jax.sharding import PartitionSpec as P

MESH = pl.DeviceIdType.MESH
F32 = jnp.float32
DEPTH = 4
ROW0 = 8
LANES = 128
N0, N1, N2, N3, N4 = 10, 18, 16, 24, 30

OFFSETS = [(b, c, a) for a in (-1, 0, 1) for b in (-1, 0, 1) for c in (-1, 0, 1) if (a, b, c) != (0, 0, 0)]


def lane_of(shape):
    return lax.broadcasted_iota(jnp.int32, shape, len(shape) - 1)


def repeat(count, body):
    lax.fori_loop(0, count, lambda i, carry: (body(i), carry)[1], 0, unroll=count)


def turn_lanes(v, by):
    return pltpu.roll(v, -by % LANES, v.ndim - 1)


def shift_x(v, c):
    return turn_lanes(v, 2 * c)


def kernel(dims, u_in, f_in, k_in, w_in, om_in, out_ref,
           ext, temp, coef, nat, stage, zsend, zrecv, dsend, drecv,
           send_sem, recv_sem, here_sem, pair_send, pair_recv, w_ref, om_ref, scalar_sem):
    n_y, n_z, ny, nz, sweeps, tiles = dims
    s = DEPTH
    half = LANES // 2
    lo, hi = ROW0, ROW0 + nz
    qe = ny + 2 * s
    first = lo - s
    bx = u_in.shape[0]

    core = lax.axis_index("gx")
    gy = lax.axis_index("gy")
    gz = lax.axis_index("gz")
    zhi, zlo = lax.rem(gz + 1, n_z), lax.rem(gz + n_z - 1, n_z)
    other = 1 - core
    yhi = lax.rem(gy + core, n_y)
    ylo = lax.rem(gy + n_y - other, n_y)

    neighbours = [
        {"gx": other, "gy": yhi, "gz": zhi}, {"gx": other, "gy": ylo, "gz": zhi},
        {"gx": other, "gy": yhi, "gz": zlo}, {"gx": other, "gy": ylo, "gz": zlo},
        {"gz": zhi}, {"gz": zlo}, {"gx": other, "gy": yhi}, {"gx": other, "gy": ylo},
    ]

    barrier = pltpu.get_barrier_semaphore()
    for nb in neighbours:
        pl.semaphore_signal(barrier, inc=1, device_id=nb, device_id_type=MESH)

    mine = pl.multiple_of(core * ny, ny)
    theirs = pl.multiple_of(other * ny, ny)
    my_x = pl.ds(core * bx, bx)
    kap, frc = 2, 3
    fields = (u_in, k_in, f_in)
    kept = [pltpu.make_async_copy(src.at[:, pl.ds(mine, ny)], nat.at[i, my_x], here_sem.at[i])
            for i, src in enumerate(fields)]

    def give(i, yt):
        return pltpu.make_async_remote_copy(
            src_ref=fields[i].at[:, pl.ds(pl.multiple_of(theirs + yt * 8, 8), 8)],
            dst_ref=nat.at[i, my_x, pl.ds(pl.multiple_of(yt * 8, 8), 8)], send_sem=pair_send.at[i, yt],
            recv_sem=pair_recv.at[i, yt], device_id={"gx": other}, device_id_type=MESH)

    for i in (1, 2, 0):
        kept[i].start()
    scalars = [pltpu.make_async_copy(w_in, w_ref, scalar_sem.at[0]), pltpu.make_async_copy(om_in, om_ref, scalar_sem.at[1])]
    for cp in scalars:
        cp.start()

    hq = ny // 2

    def copies(arr, slot, which):
        pieces = [(dsend.at[slot, i], drecv.at[slot, i]) for i in range(4)] + [
            (zsend.at[slot, 0], zrecv.at[slot, 0]),
            (zsend.at[slot, 1], zrecv.at[slot, 1]),
            (ext.at[arr, pl.ds(ny, s), pl.ds(lo, nz)], ext.at[arr, pl.ds(0, s), pl.ds(lo, nz)]),
            (ext.at[arr, pl.ds(s, s), pl.ds(lo, nz)], ext.at[arr, pl.ds(ny + s, s), pl.ds(lo, nz)]),
        ]
        return [
            pltpu.make_async_remote_copy(
                src_ref=pieces[i][0], dst_ref=pieces[i][1], send_sem=send_sem.at[slot, i],
                recv_sem=recv_sem.at[slot, i], device_id=neighbours[i], device_id_type=MESH)
            for i in which
        ]

    CORNERS, Z_FACES, Y_FACES = (0, 1, 2, 3), (4, 5), (6, 7)
    left = lane_of((s, LANES)) % 2 == 0
    below, bottom, top, above = (pl.ds(row, s) for row in (lo - s, lo, hi - s, hi))

    def swap(v):
        return jnp.where(left, turn_lanes(v, 1), turn_lanes(v, -1))

    def part(q):
        return pl.ds(q * s, s)

    low_rows = lax.broadcasted_iota(jnp.int32, (8, LANES), 0) < s
    left_tile = lane_of((8, LANES)) % 2 == 0

    def begin_z(arr, slot):
        def pack(q):
            pairs = []
            for row in (s + q, s + q + hq):
                ends = jnp.where(low_rows, ext[arr, row, pl.ds(lo, 8)], ext[arr, row, pl.ds(hi - 8, 8)])
                swapped = jnp.where(left_tile, turn_lanes(ends, 1), turn_lanes(ends, -1))
                ext[arr, row, below] = swapped[s:]
                ext[arr, row, above] = swapped[:s]
                pairs.append((ends, swapped))
            (ends_0, swapped_0), (ends_1, swapped_1) = pairs
            zsend[slot, 0, part(q)] = jnp.where(left, swapped_0[s:], ends_1[s:])
            zsend[slot, 1, part(q)] = jnp.where(left, ends_0[:s], swapped_1[:s])

        def corner(q):
            for i, (q0, rows) in enumerate(((ny, below), (s, below), (ny, above), (s, above))):
                dsend[slot, i, part(q)] = ext[arr, q0 + q, rows]

        repeat(hq, pack)
        for cp in copies(arr, slot, Z_FACES):
            cp.start()
        repeat(s, corner)
        for cp in copies(arr, slot, CORNERS):
            cp.start()

    def begin_y(arr, slot):
        for cp in copies(arr, slot, Y_FACES):
            cp.start()

    def finish_z(arr, slot):
        for cp in copies(arr, slot, Z_FACES):
            cp.wait()

        def fill(q):
            low, high = zrecv[slot, 0, part(q)], zrecv[slot, 1, part(q)]
            ext[arr, s + q, below] = jnp.where(left, low, ext[arr, s + q, below])
            ext[arr, s + q, above] = jnp.where(left, ext[arr, s + q, above], swap(high))
            ext[arr, s + q + hq, below] = jnp.where(left, swap(low), ext[arr, s + q + hq, below])
            ext[arr, s + q + hq, above] = jnp.where(left, ext[arr, s + q + hq, above], high)

        repeat(hq, fill)

    def finish_y(arr, slot):
        for cp in copies(arr, slot, CORNERS + Y_FACES):
            cp.wait()

        def fill(q):
            for i, q0 in ((0, 0), (1, s + ny)):
                ext[arr, q0 + q, below] = jnp.where(left, drecv[slot, i, part(q)], swap(ext[arr, q0 + q, top]))
                ext[arr, q0 + q, above] = jnp.where(left, swap(ext[arr, q0 + q, bottom]), drecv[slot, i + 2, part(q)])

        repeat(s, fill)

    pl.semaphore_wait(barrier, len(neighbours))
    for i in (1, 2, 0):
        for yt in range(ny // 8):
            give(i, yt).start()

    @pl.loop(0, 3)
    def _(turn):
        i = lax.rem(turn + 1, 3)
        arr = i + lax.div(i + 1, 2)
        pltpu.make_async_copy(u_in.at[:, pl.ds(mine, ny)], nat.at[i, my_x], here_sem.at[i]).wait()
        @pl.loop(0, ny // 8)
        def _(yt):
            pltpu.make_async_remote_copy(
                src_ref=u_in.at[:, pl.ds(0, 8)], dst_ref=nat.at[i, my_x, pl.ds(pl.multiple_of(yt * 8, 8), 8)],
                send_sem=pair_send.at[i, yt], recv_sem=pair_recv.at[i, yt], device_id={"gx": other},
                device_id_type=MESH).wait()
            y0 = pl.multiple_of(yt * 8, 8)
            planes = jnp.swapaxes(nat[i, :, pl.ds(y0, 8), :], 0, 1)
            for y in range(8):
                stage[y, pl.ds(0, half, stride=2), pl.ds(0, nz)] = planes[y][:, :nz]
                stage[y, pl.ds(1, half, stride=2), pl.ds(0, nz)] = planes[y][:, nz:]
                ext[arr, s + y0 + y, pl.ds(lo, nz)] = stage[y, :, pl.ds(0, nz)].T

        begin_z(arr, arr)
        begin_y(arr, arr)

    every = tuple(range(tiles))
    inner = tuple(t for t in every if first + 8 * t > lo and first + 8 * t + 8 < hi)
    outer = tuple(t for t in every if t not in inner)
    for cp in scalars:
        cp.wait()
    half_w = [0.5 * w_ref[m] for m in range(len(OFFSETS))]
    w_sum = functools.reduce(lambda x, y: x + y, half_w)

    def coefficients(which, q_lo, n, trips, stride):
        @pl.loop(0, trips)
        def _(trip):
            q0 = q_lo + trip * stride
            for t in which:
                base = first + 8 * t
                rows = {b: ext[kap, pl.ds(q0 - 1, n + 2), pl.ds(base + b, 8)] for b in (-1, 0, 1)}
                near = {(a, b): rows[b][1 + a:1 + a + n] for a in (-1, 0, 1) for b in (-1, 0, 1)}
                mid = near[0, 0]
                sums = {0: w_sum * mid}
                for m, (a, b, c) in enumerate(OFFSETS):
                    d = half_w[m] * near[a, b]
                    sums[c] = d if c not in sums else sums[c] + d
                inv = 1.0 / (sums[0] + shift_x(sums[1], 1) + shift_x(sums[-1], -1))
                mids = {0: mid, 1: shift_x(mid, -1), -1: shift_x(mid, 1)}
                invs = {0: inv, 1: shift_x(inv, -1), -1: shift_x(inv, 1)}
                for m, (a, b, c) in enumerate(OFFSETS):
                    coef[pl.ds(q0 - 1, n), t, m] = half_w[m] * (mids[c] + near[a, b]) * invs[c]
                coef[pl.ds(q0 - 1, n), t, len(OFFSETS)] = ext[frc, pl.ds(q0, n), pl.ds(base, 8)] * inv

    CN = 6
    coefficients(inner, s + 1, CN, (ny - 2) // CN, CN)

    def update(src, dst, relax, which, q_lo, n, trips, stride=None):
        @pl.loop(0, trips)
        def _(trip):
            q0 = q_lo + trip * (stride or n)
            for t in which:
                base = first + 8 * t
                rows = {b: src[pl.ds(q0 - 1, n + 2), pl.ds(base + b, 8)] for b in (-1, 0, 1)}
                sums = {0: coef[pl.ds(q0 - 1, n), t, len(OFFSETS)]}
                for m, (a, b, c) in enumerate(OFFSETS):
                    p = coef[pl.ds(q0 - 1, n), t, m] * rows[b][1 + a:1 + a + n]
                    sums[c] = p if c not in sums else sums[c] + p
                total = sums[0] + shift_x(sums[1], 1) + shift_x(sums[-1], -1)
                mid = rows[0][1:1 + n]
                dst[pl.ds(q0, n), pl.ds(base, 8)] = mid + relax * (total - mid)

    groups = sweeps // s

    @pl.loop(0, groups)
    def _(i):
        slot = lax.rem(i, 2)
        arr, nxt = ext.at[slot], ext.at[1 - slot]
        bufs = [arr, temp]
        relax = om_ref[s * i]
        update(arr, temp, relax, inner, s + 1, N0, (ny - 2) // N0)

        @pl.when(i == 0)
        def _():
            @pl.loop(kap, frc + 1)
            def _(field):
                finish_z(field, field)
                finish_y(field, field)

            coefficients(outer, s + 1, CN, (ny - 2) // CN, CN)
            coefficients(every, 1, s, 2, qe - 2 - s)

        finish_z(slot, slot)
        update(arr, temp, relax, outer, s + 1, N4, (ny - 2) // N4)
        finish_y(slot, slot)
        update(arr, temp, relax, every, 1, s, 2, qe - 2 - s)
        for j in range(1, s - 1):
            rows_now = qe - 2 - 2 * j
            update(bufs[j % 2], bufs[(j + 1) % 2], om_ref[s * i + j], every, 1 + j, N1, -(-rows_now // N1))
        src, relax = bufs[(s - 1) % 2], om_ref[s * i + s - 1]
        update(src, nxt, relax, outer, s, N2, ny // N2)

        @pl.when(i < groups - 1)
        def _():
            begin_z(1 - slot, 1 - slot)

        update(src, nxt, relax, inner, s, s, 2, ny - s)

        @pl.when(i < groups - 1)
        def _():
            begin_y(1 - slot, 1 - slot)

        update(src, nxt, relax, inner, 2 * s, N3, (ny - 2 * s) // N3)

    last = groups % 2

    def home(yt):
        rows = pl.ds(pl.multiple_of(core * ny + yt * 8, 8), 8)
        return (pltpu.make_async_copy(
                    nat.at[0, my_x, pl.ds(pl.multiple_of(yt * 8, 8), 8)], out_ref.at[:, rows], here_sem.at[yt]),
                pltpu.make_async_remote_copy(
                    src_ref=nat.at[0, pl.ds(other * bx, bx), pl.ds(pl.multiple_of(yt * 8, 8), 8)], dst_ref=out_ref.at[:, rows],
                    send_sem=pair_send.at[0, yt], recv_sem=pair_recv.at[0, yt], device_id={"gx": other},
                    device_id_type=MESH))

    @pl.loop(0, ny // 8)
    def _(step):
        yt = pl.multiple_of(step * 8, 8)
        planes = []
        for y in range(8):
            stage[y, :, pl.ds(0, nz)] = ext[last, s + yt + y, pl.ds(lo, nz)].T
            planes.append(jnp.concatenate([stage[y, pl.ds(0, half, stride=2), pl.ds(0, nz)],
                                           stage[y, pl.ds(1, half, stride=2), pl.ds(0, nz)]], axis=1))
        nat[0, :, pl.ds(yt, 8), :] = jnp.swapaxes(jnp.stack(planes), 0, 1)
        for cp in home(step):
            cp.start()

    @pl.loop(0, ny // 8)
    def _(step):
        for cp in home(step):
            cp.wait()


def solution(mesh):
    spec = P(("batch", "gx"), "gy", "gz")
    n_x, n_y, n_z = mesh.shape["gx"], mesh.shape["gy"], mesh.shape["gz"]

    def local(u, f, k, w, om):
        bx, by, bz = u.shape
        ny, nz = by // n_x, bz // 2
        s = DEPTH
        tiles = -(-(nz + 2 * s - 1) // 8)
        rows = ROW0 + -(-(nz + s) // 8) * 8
        qe = ny + 2 * s
        hbm = pl.BlockSpec(memory_space=pl.ANY)
        dma = pltpu.SemaphoreType.DMA
        return pl.pallas_call(
            functools.partial(kernel, (n_y, n_z, ny, nz, om.shape[0], tiles)),
            out_shape=jax.ShapeDtypeStruct(u.shape, F32),
            in_specs=[hbm, hbm, hbm, hbm, hbm],
            out_specs=hbm,
            scratch_shapes=[
                pltpu.VMEM((4, qe, rows, LANES), F32),
                pltpu.VMEM((qe, rows, LANES), F32),
                pltpu.VMEM((qe - 2, tiles, len(OFFSETS) + 2, 8, LANES), F32),
                pltpu.VMEM((3, n_x * bx, ny, bz), F32),
                pltpu.VMEM((8, LANES, LANES), F32),
                pltpu.VMEM((4, 2, ny // 2 * s, LANES), F32),
                pltpu.VMEM((4, 2, ny // 2 * s, LANES), F32),
                pltpu.VMEM((4, 4, s * s, LANES), F32),
                pltpu.VMEM((4, 4, s * s, LANES), F32),
                dma((4, 8)), dma((4, 8)), dma((4,)), dma((3, ny // 8)), dma((3, ny // 8)),
                pltpu.SMEM(w.shape, F32), pltpu.SMEM(om.shape, F32), dma((2,)),
            ],
            compiler_params=pltpu.CompilerParams(collective_id=0, has_side_effects=True, vmem_limit_bytes=56 << 20),
        )(u, f, k, w, om)

    return jax.shard_map(local, mesh=mesh, in_specs=(spec, spec, spec, P(), P()), out_specs=spec, check_vma=False)
```

```python
import functools

import jax
import jax.numpy as jnp
from jax import lax
from jax.experimental import pallas as pl
from jax.experimental.pallas import tpu as pltpu
from jax.sharding import PartitionSpec as P

MESH = pl.DeviceIdType.MESH
F32 = jnp.float32
DEPTH = 4
ROW0 = 8
LANES = 128
N0, N1, N2, N3, N4 = 30, 18, 16, 24, 30

OFFSETS = [(b, c, a) for a in (-1, 0, 1) for b in (-1, 0, 1) for c in (-1, 0, 1) if (a, b, c) != (0, 0, 0)]


def lane_of(shape):
    return lax.broadcasted_iota(jnp.int32, shape, len(shape) - 1)


def repeat(count, body):
    lax.fori_loop(0, count, lambda i, carry: (body(i), carry)[1], 0, unroll=count)


def turn_lanes(v, by):
    return pltpu.roll(v, -by % LANES, v.ndim - 1)


def shift_x(v, c):
    return turn_lanes(v, 2 * c)


def kernel(dims, u_in, f_in, k_in, w_in, om_in, out_ref,
           ext, temp, coef, nat, stage, zsend, zrecv, dsend, drecv,
           send_sem, recv_sem, here_sem, pair_send, pair_recv, w_ref, om_ref, scalar_sem):
    n_y, n_z, ny, nz, sweeps, tiles = dims
    s = DEPTH
    half = LANES // 2
    lo, hi = ROW0, ROW0 + nz
    qe = ny + 2 * s
    first = lo - s
    bx = u_in.shape[0]

    core = lax.axis_index("gx")
    gy = lax.axis_index("gy")
    gz = lax.axis_index("gz")
    zhi, zlo = lax.rem(gz + 1, n_z), lax.rem(gz + n_z - 1, n_z)
    other = 1 - core
    yhi = lax.rem(gy + core, n_y)
    ylo = lax.rem(gy + n_y - other, n_y)

    neighbours = [
        {"gx": other, "gy": yhi, "gz": zhi}, {"gx": other, "gy": ylo, "gz": zhi},
        {"gx": other, "gy": yhi, "gz": zlo}, {"gx": other, "gy": ylo, "gz": zlo},
        {"gz": zhi}, {"gz": zlo}, {"gx": other, "gy": yhi}, {"gx": other, "gy": ylo},
    ]

    barrier = pltpu.get_barrier_semaphore()
    for nb in neighbours:
        pl.semaphore_signal(barrier, inc=1, device_id=nb, device_id_type=MESH)

    mine = pl.multiple_of(core * ny, ny)
    theirs = pl.multiple_of(other * ny, ny)
    my_x = pl.ds(core * bx, bx)
    kap, frc = 2, 3
    fields = (u_in, k_in, f_in)
    kept = [pltpu.make_async_copy(src.at[:, pl.ds(mine, ny)], nat.at[i, my_x], here_sem.at[i])
            for i, src in enumerate(fields)]

    def give(i, yt):
        return pltpu.make_async_remote_copy(
            src_ref=fields[i].at[:, pl.ds(pl.multiple_of(theirs + yt * 8, 8), 8)],
            dst_ref=nat.at[i, my_x, pl.ds(pl.multiple_of(yt * 8, 8), 8)], send_sem=pair_send.at[i, yt],
            recv_sem=pair_recv.at[i, yt], device_id={"gx": other}, device_id_type=MESH)

    for i in (1, 2, 0):
        kept[i].start()
    scalars = [pltpu.make_async_copy(w_in, w_ref, scalar_sem.at[0]), pltpu.make_async_copy(om_in, om_ref, scalar_sem.at[1])]
    for cp in scalars:
        cp.start()

    hq = ny // 2

    def copies(arr, slot, which):
        pieces = [(dsend.at[slot, i], drecv.at[slot, i]) for i in range(4)] + [
            (zsend.at[slot, 0], zrecv.at[slot, 0]),
            (zsend.at[slot, 1], zrecv.at[slot, 1]),
            (ext.at[arr, pl.ds(ny, s), pl.ds(lo, nz)], ext.at[arr, pl.ds(0, s), pl.ds(lo, nz)]),
            (ext.at[arr, pl.ds(s, s), pl.ds(lo, nz)], ext.at[arr, pl.ds(ny + s, s), pl.ds(lo, nz)]),
        ]
        return [
            pltpu.make_async_remote_copy(
                src_ref=pieces[i][0], dst_ref=pieces[i][1], send_sem=send_sem.at[slot, i],
                recv_sem=recv_sem.at[slot, i], device_id=neighbours[i], device_id_type=MESH)
            for i in which
        ]

    CORNERS, Z_FACES, Y_FACES = (0, 1, 2, 3), (4, 5), (6, 7)
    left = lane_of((s, LANES)) % 2 == 0
    below, bottom, top, above = (pl.ds(row, s) for row in (lo - s, lo, hi - s, hi))

    def swap(v):
        return jnp.where(left, turn_lanes(v, 1), turn_lanes(v, -1))

    def part(q):
        return pl.ds(q * s, s)

    low_rows = lax.broadcasted_iota(jnp.int32, (8, LANES), 0) < s
    left_tile = lane_of((8, LANES)) % 2 == 0

    def begin_z(arr, slot):
        def pack(q):
            pairs = []
            for row in (s + q, s + q + hq):
                ends = jnp.where(low_rows, ext[arr, row, pl.ds(lo, 8)], ext[arr, row, pl.ds(hi - 8, 8)])
                swapped = jnp.where(left_tile, turn_lanes(ends, 1), turn_lanes(ends, -1))
                ext[arr, row, below] = swapped[s:]
                ext[arr, row, above] = swapped[:s]
                pairs.append((ends, swapped))
            (ends_0, swapped_0), (ends_1, swapped_1) = pairs
            zsend[slot, 0, part(q)] = jnp.where(left, swapped_0[s:], ends_1[s:])
            zsend[slot, 1, part(q)] = jnp.where(left, ends_0[:s], swapped_1[:s])

        def corner(q):
            for i, (q0, rows) in enumerate(((ny, below), (s, below), (ny, above), (s, above))):
                dsend[slot, i, part(q)] = ext[arr, q0 + q, rows]

        repeat(hq, pack)
        for cp in copies(arr, slot, Z_FACES):
            cp.start()
        repeat(s, corner)
        for cp in copies(arr, slot, CORNERS):
            cp.start()

    def begin_y(arr, slot):
        for cp in copies(arr, slot, Y_FACES):
            cp.start()

    def finish_z(arr, slot):
        for cp in copies(arr, slot, Z_FACES):
            cp.wait()

        def fill(q):
            low, high = zrecv[slot, 0, part(q)], zrecv[slot, 1, part(q)]
            ext[arr, s + q, below] = jnp.where(left, low, ext[arr, s + q, below])
            ext[arr, s + q, above] = jnp.where(left, ext[arr, s + q, above], swap(high))
            ext[arr, s + q + hq, below] = jnp.where(left, swap(low), ext[arr, s + q + hq, below])
            ext[arr, s + q + hq, above] = jnp.where(left, ext[arr, s + q + hq, above], high)

        repeat(hq, fill)

    def finish_y(arr, slot):
        for cp in copies(arr, slot, CORNERS + Y_FACES):
            cp.wait()

        def fill(q):
            for i, q0 in ((0, 0), (1, s + ny)):
                ext[arr, q0 + q, below] = jnp.where(left, drecv[slot, i, part(q)], swap(ext[arr, q0 + q, top]))
                ext[arr, q0 + q, above] = jnp.where(left, swap(ext[arr, q0 + q, bottom]), drecv[slot, i + 2, part(q)])

        repeat(s, fill)

    pl.semaphore_wait(barrier, len(neighbours))
    for i in (1, 2, 0):
        for yt in range(ny // 8):
            give(i, yt).start()

    @pl.loop(0, 3)
    def _(turn):
        i = lax.rem(turn + 1, 3)
        arr = i + lax.div(i + 1, 2)
        pltpu.make_async_copy(u_in.at[:, pl.ds(mine, ny)], nat.at[i, my_x], here_sem.at[i]).wait()
        @pl.loop(0, ny // 8)
        def _(yt):
            pltpu.make_async_remote_copy(
                src_ref=u_in.at[:, pl.ds(0, 8)], dst_ref=nat.at[i, my_x, pl.ds(pl.multiple_of(yt * 8, 8), 8)],
                send_sem=pair_send.at[i, yt], recv_sem=pair_recv.at[i, yt], device_id={"gx": other},
                device_id_type=MESH).wait()
            y0 = pl.multiple_of(yt * 8, 8)
            planes = jnp.swapaxes(nat[i, :, pl.ds(y0, 8), :], 0, 1)
            for y in range(8):
                stage[y, pl.ds(0, half, stride=2), pl.ds(0, nz)] = planes[y][:, :nz]
                stage[y, pl.ds(1, half, stride=2), pl.ds(0, nz)] = planes[y][:, nz:]
                ext[arr, s + y0 + y, pl.ds(lo, nz)] = stage[y, :, pl.ds(0, nz)].T

        begin_z(arr, arr)
        begin_y(arr, arr)

    every = tuple(range(tiles))
    inner = tuple(t for t in every if first + 8 * t > lo and first + 8 * t + 8 < hi)
    outer = tuple(t for t in every if t not in inner)
    for cp in scalars:
        cp.wait()
    half_w = [0.5 * w_ref[m] for m in range(len(OFFSETS))]
    w_sum = functools.reduce(lambda x, y: x + y, half_w)

    def coefficients(which, q_lo, n, trips, stride):
        @pl.loop(0, trips)
        def _(trip):
            q0 = q_lo + trip * stride
            for t in which:
                base = first + 8 * t
                rows = {b: ext[kap, pl.ds(q0 - 1, n + 2), pl.ds(base + b, 8)] for b in (-1, 0, 1)}
                near = {(a, b): rows[b][1 + a:1 + a + n] for a in (-1, 0, 1) for b in (-1, 0, 1)}
                mid = near[0, 0]
                sums = {0: w_sum * mid}
                for m, (a, b, c) in enumerate(OFFSETS):
                    d = half_w[m] * near[a, b]
                    sums[c] = d if c not in sums else sums[c] + d
                inv = 1.0 / (sums[0] + shift_x(sums[1], 1) + shift_x(sums[-1], -1))
                mids = {0: mid, 1: shift_x(mid, -1), -1: shift_x(mid, 1)}
                invs = {0: inv, 1: shift_x(inv, -1), -1: shift_x(inv, 1)}
                for m, (a, b, c) in enumerate(OFFSETS):
                    coef[pl.ds(q0 - 1, n), t, m] = half_w[m] * (mids[c] + near[a, b]) * invs[c]
                coef[pl.ds(q0 - 1, n), t, len(OFFSETS)] = ext[frc, pl.ds(q0, n), pl.ds(base, 8)] * inv

    CN = 10
    coefficients(inner, s + 1, CN, (ny - 2) // CN, CN)

    def update(src, dst, relax, which, q_lo, n, trips, stride=None):
        @pl.loop(0, trips)
        def _(trip):
            q0 = q_lo + trip * (stride or n)
            for t in which:
                base = first + 8 * t
                rows = {b: src[pl.ds(q0 - 1, n + 2), pl.ds(base + b, 8)] for b in (-1, 0, 1)}
                sums = {0: coef[pl.ds(q0 - 1, n), t, len(OFFSETS)]}
                for m, (a, b, c) in enumerate(OFFSETS):
                    p = coef[pl.ds(q0 - 1, n), t, m] * rows[b][1 + a:1 + a + n]
                    sums[c] = p if c not in sums else sums[c] + p
                total = sums[0] + shift_x(sums[1], 1) + shift_x(sums[-1], -1)
                mid = rows[0][1:1 + n]
                dst[pl.ds(q0, n), pl.ds(base, 8)] = mid + relax * (total - mid)

    groups = sweeps // s

    @pl.loop(0, groups)
    def _(i):
        slot = lax.rem(i, 2)
        arr, nxt = ext.at[slot], ext.at[1 - slot]
        bufs = [arr, temp]
        relax = om_ref[s * i]
        update(arr, temp, relax, inner, s + 1, N0, (ny - 2) // N0)

        @pl.when(i == 0)
        def _():
            @pl.loop(kap, frc + 1)
            def _(field):
                finish_z(field, field)
                finish_y(field, field)

            coefficients(outer, s + 1, CN, (ny - 2) // CN, CN)
            coefficients(every, 1, s, 2, qe - 2 - s)

        finish_z(slot, slot)
        update(arr, temp, relax, outer, s + 1, N4, (ny - 2) // N4)
        finish_y(slot, slot)
        update(arr, temp, relax, every, 1, s, 2, qe - 2 - s)
        for j in range(1, s - 1):
            rows_now = qe - 2 - 2 * j
            update(bufs[j % 2], bufs[(j + 1) % 2], om_ref[s * i + j], every, 1 + j, N1, -(-rows_now // N1))
        src, relax = bufs[(s - 1) % 2], om_ref[s * i + s - 1]
        update(src, nxt, relax, outer, s, N2, ny // N2)

        @pl.when(i < groups - 1)
        def _():
            begin_z(1 - slot, 1 - slot)

        update(src, nxt, relax, inner, s, s, 2, ny - s)

        @pl.when(i < groups - 1)
        def _():
            begin_y(1 - slot, 1 - slot)

        update(src, nxt, relax, inner, 2 * s, N3, (ny - 2 * s) // N3)

    last = groups % 2

    def home(yt):
        rows = pl.ds(pl.multiple_of(core * ny + yt * 8, 8), 8)
        return (pltpu.make_async_copy(
                    nat.at[0, my_x, pl.ds(pl.multiple_of(yt * 8, 8), 8)], out_ref.at[:, rows], here_sem.at[yt]),
                pltpu.make_async_remote_copy(
                    src_ref=nat.at[0, pl.ds(other * bx, bx), pl.ds(pl.multiple_of(yt * 8, 8), 8)], dst_ref=out_ref.at[:, rows],
                    send_sem=pair_send.at[0, yt], recv_sem=pair_recv.at[0, yt], device_id={"gx": other},
                    device_id_type=MESH))

    @pl.loop(0, ny // 8)
    def _(step):
        yt = pl.multiple_of(step * 8, 8)
        planes = []
        for y in range(8):
            stage[y, :, pl.ds(0, nz)] = ext[last, s + yt + y, pl.ds(lo, nz)].T
            planes.append(jnp.concatenate([stage[y, pl.ds(0, half, stride=2), pl.ds(0, nz)],
                                           stage[y, pl.ds(1, half, stride=2), pl.ds(0, nz)]], axis=1))
        nat[0, :, pl.ds(yt, 8), :] = jnp.swapaxes(jnp.stack(planes), 0, 1)
        for cp in home(step):
            cp.start()

    @pl.loop(0, ny // 8)
    def _(step):
        for cp in home(step):
            cp.wait()


def solution(mesh):
    spec = P(("batch", "gx"), "gy", "gz")
    n_x, n_y, n_z = mesh.shape["gx"], mesh.shape["gy"], mesh.shape["gz"]

    def local(u, f, k, w, om):
        bx, by, bz = u.shape
        ny, nz = by // n_x, bz // 2
        s = DEPTH
        tiles = -(-(nz + 2 * s - 1) // 8)
        rows = ROW0 + -(-(nz + s) // 8) * 8
        qe = ny + 2 * s
        hbm = pl.BlockSpec(memory_space=pl.ANY)
        dma = pltpu.SemaphoreType.DMA
        return pl.pallas_call(
            functools.partial(kernel, (n_y, n_z, ny, nz, om.shape[0], tiles)),
            out_shape=jax.ShapeDtypeStruct(u.shape, F32),
            in_specs=[hbm, hbm, hbm, hbm, hbm],
            out_specs=hbm,
            scratch_shapes=[
                pltpu.VMEM((4, qe, rows, LANES), F32),
                pltpu.VMEM((qe, rows, LANES), F32),
                pltpu.VMEM((qe - 2, tiles, len(OFFSETS) + 2, 8, LANES), F32),
                pltpu.VMEM((3, n_x * bx, ny, bz), F32),
                pltpu.VMEM((8, LANES, LANES), F32),
                pltpu.VMEM((4, 2, ny // 2 * s, LANES), F32),
                pltpu.VMEM((4, 2, ny // 2 * s, LANES), F32),
                pltpu.VMEM((4, 4, s * s, LANES), F32),
                pltpu.VMEM((4, 4, s * s, LANES), F32),
                dma((4, 8)), dma((4, 8)), dma((4,)), dma((3, ny // 8)), dma((3, ny // 8)),
                pltpu.SMEM(w.shape, F32), pltpu.SMEM(om.shape, F32), dma((2,)),
            ],
            compiler_params=pltpu.CompilerParams(collective_id=0, has_side_effects=True, vmem_limit_bytes=56 << 20),
        )(u, f, k, w, om)

    return jax.shard_map(local, mesh=mesh, in_specs=(spec, spec, spec, P(), P()), out_specs=spec, check_vma=False)
```
